128 devices in a mesh: slab: 4 (over y_hi, core), pencil: 32 (over y_lo, x, z).
Axes of the slice: x: 4, y: 4 (y_hi: 2, y_lo: 2; y = y_hi * 2 + y_lo), z: 4, core: 2. Of those that a mesh axis runs over, the one named last changes fastest.
Arguments:
- density: float32 [512, 768, 512], P('pencil', None, 'slab'), may hold values from -6 to 6
- source: float32 [512, 768, 512], P('pencil', None, 'slab'), may hold values from -6 to 8
- coupling: float32 [3], replicated, may hold values from 0.25 to 2, as said below
- width_inverse: float32 [6, 128, 128], replicated, as said below
- height_inverse: float32 [4, 128, 128], replicated, as said below
- depth_inverse: float32 [4, 128, 128], replicated, as said below
Outputs:
- stepped: float32 [512, 768, 512], P('pencil', None, 'slab')
The draws below stay inside these ranges and needn't reach their ends.
Inputs may be any that keep to these rules, and one draw needn't show every extreme that they name: coupling holds three positive coefficients. `width_inverse`: block i is the inverse of the i-th pivot block of the block LU factorization of the tridiagonal line matrix with diagonal 1 + 2 s and off-diagonals -s, s the matching coupling. `height_inverse`: as for width_inverse, for the height lines. `depth_inverse`: as for width_inverse, for the depth lines.
All inputs are finite; a program needn't handle non-finite values.
Results may differ from the reference program's by a relative error of at most 0.00027.
Values sent between devices are 32-bit elements; how exact they have to be, the bound alone decides.
No kernel may reach another device: no remote copies, remote signals or barrier semaphores. Data moves between devices by JAX's collectives and lax.ppermute only.
A program may use at most 128 MiB of HBM per device.

```python
import jax
import jax.numpy as jnp
from jax import lax

BLOCK = 128
NX = 768
NY = 512
NZ = 512


def coupling_values(key):
    folded = jax.random.fold_in(key, 7)
    uniform_draw = jax.random.uniform(folded, (3,), jnp.float32)
    return 0.25 * jnp.exp(uniform_draw * jnp.log(8.0))


def block_inverses(strength, count):
    identity = jnp.eye(BLOCK, dtype=jnp.float32)
    beside = jnp.eye(BLOCK, k=1, dtype=jnp.float32) + jnp.eye(BLOCK, k=-1, dtype=jnp.float32)
    tridiag = (1.0 + 2.0 * strength) * identity - strength * beside
    corner_unit = jnp.zeros((BLOCK, BLOCK), jnp.float32).at[0, 0].set(1.0)
    matrices = []
    corner = jnp.float32(0.0)
    for number in range(count):
        pivot = tridiag - strength * strength * corner * corner_unit
        inverse = jnp.linalg.inv(pivot)
        matrices.append(inverse)
        corner = inverse[BLOCK - 1, BLOCK - 1]
    return jnp.stack(matrices)


def draw_source(key, part):
    rough = jnp.clip(jax.random.normal(jax.random.fold_in(key, 11), (NY, NX, NZ), jnp.float32), -6.0, 6.0)
    return rough


def draw_coupling(key, part):
    return coupling_values(key)


def draw_width_inverse(key, part):
    return block_inverses(coupling_values(key)[0], NX // BLOCK)


def draw_height_inverse(key, part):
    return block_inverses(coupling_values(key)[1], NY // BLOCK)


def draw_depth_inverse(key, part):
    return block_inverses(coupling_values(key)[2], NZ // BLOCK)


def levels(own_key, dims, split, low, largest):
    def one(position, parts):
        heights = jax.random.uniform(jax.random.fold_in(jax.random.fold_in(own_key, 6), position), (parts,), jnp.float32, low / len(split), largest / len(split))
        return jnp.repeat(jnp.exp(heights), dims[position] // parts).reshape((-1,) + (1,) * (len(dims) - position - 1))

    gain = one(*split[0])
    for cut in split[1:]:
        gain = gain * one(*cut)
    return gain


def bell_draw(own_key, extent, deviation, most, pieces=(), kind=jnp.bfloat16):
    values = jax.random.normal(own_key, extent, jnp.float32) * deviation
    if len(pieces) > 0:
        values = levels(own_key, extent, pieces, -0.22, 0.18) * values
    return jnp.clip(values, min=-most, max=most).astype(kind)


def setup_inputs(seed: int = 0) -> dict:
    streams_of = jax.random.split(jax.random.key(seed), 7)
    return {
        "density": bell_draw(streams_of[0], (NY, NX, NZ), 1.0, 6.0, ((0, 32), (2, 4)), jnp.float32),
        "source": draw_source(jax.random.fold_in(streams_of[6], 71), 0),
        "coupling": draw_coupling(jax.random.fold_in(streams_of[6], 71), 0),
        "width_inverse": draw_width_inverse(jax.random.fold_in(streams_of[6], 71), 0),
        "height_inverse": draw_height_inverse(jax.random.fold_in(streams_of[6], 71), 0),
        "depth_inverse": draw_depth_inverse(jax.random.fold_in(streams_of[6], 71), 0),
    }


def solve_inner(rhs, inverses, strength):
    outer, length, inner = rhs.shape
    size = inverses.shape[1]
    count = length // size
    blocked = rhs.reshape(outer, count, size, inner)

    def forward(current, state):
        result, carry = state
        piece = lax.dynamic_index_in_dim(blocked, current, 1, keepdims=False)
        matrix = lax.dynamic_index_in_dim(inverses, current, 0, keepdims=False)
        value = jnp.einsum('pkq,jk->pjq', piece, matrix, precision=lax.Precision.HIGHEST)
        value = value + strength * matrix[:, 0][None, :, None] * carry[:, None, :]
        result = lax.dynamic_update_index_in_dim(result, value, current, 1)
        return (result, value[:, size - 1, :])
    start = (jnp.zeros_like(blocked), jnp.zeros((outer, inner), blocked.dtype))
    halfway, unused = lax.fori_loop(0, count, forward, start)

    def backward(step, state):
        result, carry = state
        current = count - 1 - step
        value = lax.dynamic_index_in_dim(result, current, 1, keepdims=False)
        matrix = lax.dynamic_index_in_dim(inverses, current, 0, keepdims=False)
        value = value + strength * matrix[:, size - 1][None, :, None] * carry[:, None, :]
        result = lax.dynamic_update_index_in_dim(result, value, current, 1)
        return (result, value[:, 0, :])
    final, unused = lax.fori_loop(0, count, backward, (halfway, jnp.zeros((outer, inner), blocked.dtype)))
    return final.reshape(outer, length, inner)

def solve_last(rhs, inverses, strength):
    rows, length = rhs.shape
    size = inverses.shape[1]
    count = length // size
    blocked = rhs.reshape(rows, count, size)

    def forward(current, state):
        result, carry = state
        piece = lax.dynamic_index_in_dim(blocked, current, 1, keepdims=False)
        matrix = lax.dynamic_index_in_dim(inverses, current, 0, keepdims=False)
        value = jnp.einsum('pk,jk->pj', piece, matrix, precision=lax.Precision.HIGHEST)
        value = value + strength * matrix[:, 0][None, :] * carry[:, None]
        result = lax.dynamic_update_index_in_dim(result, value, current, 1)
        return (result, value[:, size - 1])
    halfway, unused = lax.fori_loop(0, count, forward, (jnp.zeros_like(blocked), jnp.zeros((rows,), blocked.dtype)))

    def backward(step, state):
        result, carry = state
        current = count - 1 - step
        value = lax.dynamic_index_in_dim(result, current, 1, keepdims=False)
        matrix = lax.dynamic_index_in_dim(inverses, current, 0, keepdims=False)
        value = value + strength * matrix[:, size - 1][None, :] * carry[:, None]
        result = lax.dynamic_update_index_in_dim(result, value, current, 1)
        return (result, value[:, 0])
    final, unused = lax.fori_loop(0, count, backward, (halfway, jnp.zeros((rows,), blocked.dtype)))
    return final.reshape(rows, length)

def second_difference(values, axis):
    widths = [(0, 0), (0, 0), (0, 0)]
    widths[axis] = (1, 1)
    padded = jnp.pad(values, widths)
    length = values.shape[axis]
    upper = lax.slice_in_dim(padded, 2, length + 2, axis=axis)
    lower = lax.slice_in_dim(padded, 0, length, axis=axis)
    return upper + lower - 2.0 * values

def reference(density, source, coupling, width_inverse, height_inverse, depth_inverse):
    along_width = second_difference(density, 1)
    along_height = second_difference(density, 0)
    along_depth = second_difference(density, 2)
    explicit = 2.0 * (coupling[0] * along_width + coupling[1] * along_height + coupling[2] * along_depth) + source
    width_step = solve_inner(explicit, width_inverse, coupling[0])
    height_step = solve_inner(width_step.reshape(1, NY, NX * NZ), height_inverse, coupling[1]).reshape(NY, NX, NZ)
    depth_step = solve_last(height_step.reshape(NY * NX, NZ), depth_inverse, coupling[2]).reshape(NY, NX, NZ)
    return density + depth_step
```

```python
import jax
import jax.numpy as jnp
from jax import lax
from jax.experimental import pallas as pl
from jax.experimental.pallas import tpu as pltpu
from jax.sharding import PartitionSpec as P

H, W, D = 16, 768, 128
B = 128
NB = W // B
NP = 32
S = W // NP
f32 = jnp.float32
bf16 = jnp.bfloat16
HIGHEST = lax.Precision.HIGHEST


def log_decay(s):
    return jnp.log(2.0 * s / (1.0 + 2.0 * s + jnp.sqrt(1.0 + 4.0 * s)))


def pivots(log_r, length):
    return (
        jnp.exp(log_r)
        * (1.0 - jnp.exp(log_r * (2.0 * length)))
        / (1.0 - jnp.exp(log_r * (2.0 * length + 2.0)))
    )


def influence(log_r, m, i):
    return (
        jnp.exp(log_r * (i + 1.0))
        * (1.0 - jnp.exp(log_r * (2.0 * (m - i))))
        / (1.0 - jnp.exp(log_r * (2.0 * m + 2.0)))
    )


def green(s, log_r, n, i, j):
    low, high = jnp.minimum(i, j), jnp.maximum(i, j)
    return (
        jnp.exp(log_r * (high - low))
        * (1.0 - jnp.exp(log_r * (2.0 * low + 2.0)))
        * (1.0 - jnp.exp(log_r * (2.0 * (n - high))))
        / (jnp.sqrt(1.0 + 4.0 * s) * (1.0 - jnp.exp(log_r * (2.0 * n + 2.0))))
    )


def split(x):
    hi = x.astype(bf16)
    return hi, (x - hi.astype(f32)).astype(bf16)


def dot(a, b):
    return lax.dot_general(a, b, (((1,), (0,)), ((), ())), preferred_element_type=f32)


def iota(shape, dim):
    return lax.broadcasted_iota(jnp.int32, shape, dim)


HEAD, BEFORE_H, BEFORE_W, AH, CH, MH, FROM = 0, 1, 5, 9, 10, 11, 12


def tables_kernel(cpl, slab, wi, di, par, cols, rows, gw3, gd4, spread, hmat, hcol):
    row = (1, 128)
    sw, sh, sd = (jnp.full(row, cpl[k], f32) for k in range(3))
    lw, lh, ld = log_decay(sw), log_decay(sh), log_decay(sd)
    lane = iota(row, 1)
    k = lane.astype(f32)
    heads = [2.0 - 4.0 * sw - 4.0 * sd, 2.0 * sw, 2.0 * sd]
    for log_r, m in ((lw, float(B)), (lh, float(H)), (ld, float(D))):
        heads += [influence(log_r, m, 0.0), influence(log_r, m, m - 1.0)]
    head = jnp.zeros(row, f32)
    for at, v in enumerate(heads):
        head = jnp.where(lane == at, v, head)
    par[HEAD : HEAD + 1] = head
    for at, log_r, m, p, q in ((BEFORE_H, lh, float(H), heads[5], heads[6]), (BEFORE_W, lw, float(B), heads[3], heads[4])):
        before = pivots(log_r, m * k)
        inv = 1.0 / (1.0 - p * before)
        w = q * before * inv
        for n, v in enumerate((before, inv, w, q + w * p)):
            par[at + n : at + n + 1] = v
    kc = jnp.minimum(k, H - 1.0)
    ch = pivots(lh, kc + 1.0)
    par[AH : AH + 1] = influence(lh, float(H), kc)
    par[CH : CH + 1] = ch
    par[MH : MH + 1] = ch / sh
    me = slab[0]
    other = lax.bitwise_and(me - lane, 3)
    of, mf = other.astype(f32), jnp.full(row, me, jnp.int32).astype(f32)
    n = float(4 * D)
    for side, (where, beside, inside) in enumerate(
        ((D * mf - 1.0, me - 1, me > 0), (D * mf + D, me + 1, me < 3))
    ):
        spot = jnp.clip(where, 0.0, n - 1.0)
        first = jnp.where(other >= 1, sd * green(sd, ld, n, spot, jnp.maximum(D * of - 1.0, 0.0)), 0.0)
        last = jnp.where(other <= 2, sd * green(sd, ld, n, spot, jnp.minimum(D * of + D, n - 1.0)), 0.0)
        same = jnp.where(other == beside, 1.0, 0.0)
        if side == 0:
            last = last + same
        else:
            first = first + same
        par[FROM + 2 * side : FROM + 2 * side + 1] = jnp.where(inside, first, 0.0)
        par[FROM + 2 * side + 1 : FROM + 2 * side + 2] = jnp.where(inside, last, 0.0)
    tall = iota((B, D), 0).astype(f32)
    lww = jnp.broadcast_to(lw, (B, D))
    cols[0] = influence(lww, float(B), tall)
    cols[1] = influence(lww, float(B), B - 1.0 - tall)
    rows[0:1] = influence(lw, float(B), k)
    rows[1:2] = influence(lw, float(B), B - 1.0 - k)
    hi, lo = split(wi[0])
    gw3[:, :B] = hi
    gw3[:, B : 2 * B] = hi
    gw3[:, 2 * B :] = lo
    hi, lo = split(di[0].T)
    gd4[:D, :D] = hi
    gd4[:D, D:] = lo
    gd4[D:, :D] = hi
    gd4[D:, D:] = jnp.zeros((D, D), bf16)
    ad, bd = influence(ld, float(D), k), influence(ld, float(D), D - 1.0 - k)
    line = iota((2 * H, D), 0)
    for h in range(H):
        v = jnp.where(line == h, ad, jnp.where(line == H + h, bd, 0.0))
        hi, lo = split(v)
        at = slice(h * D, (h + 1) * D)
        spread[: 2 * H, at] = hi
        spread[2 * H : 4 * H, at] = hi
        spread[4 * H :, at] = lo
    a = iota((2 * H, 128), 0)
    b = iota((2 * H, 128), 1)
    af = lax.bitwise_and(a, H - 1).astype(f32)
    bfl = lax.bitwise_and(b, H - 1).astype(f32)
    wide_h = jnp.broadcast_to(lh, (2 * H, 128))
    g = green(jnp.broadcast_to(sh, (2 * H, 128)), wide_h, float(H), af, bfl)
    hmat[...] = jnp.where((b < 2 * H) & (lax.shift_right_logical(a, 4) == lax.shift_right_logical(b, 4)), g, 0.0)
    c = iota((H, 128), 0).astype(f32)
    ln = iota((H, 128), 1)
    hcol[...] = influence(jnp.broadcast_to(lh, (H, 128)), float(H), jnp.where(ln == 0, c, H - 1.0 - c))


def sums_kernel(cpl, rho, sig, cr, cs, own, comb, coef, packed):
    i = pl.program_id(0)

    @pl.when(i == 0)
    def _():
        sh = jnp.full((8, 128), cpl[1], f32)
        lh = log_decay(sh)
        for h in range(H):
            coef[h] = influence(lh, float(H), float(h)) / sh

    T = 32
    lane = iota((T, D), 1)
    packs, combs = [], []
    for t in range(B // T):
        at = slice(t * T, (t + 1) * T)
        fr = jnp.zeros((T, D), f32)
        tr, fs, ts, pack = fr, fr, fr, fr
        for h in range(H):
            x, y = rho[h, at, :], sig[h, at, :]
            cf = jnp.broadcast_to(coef[h, 0:1, :], (T, D))
            ct = jnp.broadcast_to(coef[H - 1 - h, 0:1, :], (T, D))
            fr, tr, fs, ts = fr + cf * x, tr + ct * x, fs + cf * y, ts + ct * y
            pack = jnp.where((lane == 2 * h) | (lane == 2 * h + 1), pltpu.roll(x, 2 * h + 1, 1), pack)
        cr[0, at], cr[1, at], cs[0, at], cs[1, at] = fr, tr, fs, ts
        packs.append(pack)
        combs.append(jnp.where(lane < 2, pltpu.roll(fr, 1, 1), pltpu.roll(tr, 3, 1)))
    packed[...] = jnp.concatenate(packs, axis=0).T[: 2 * H]
    own[:H] = packed[pl.ds(1, H, stride=2), :]
    own[H:] = packed[pl.ds(0, H, stride=2), :]
    comb[...] = jnp.concatenate(combs, axis=0).T[:8]


def chain_w(yf, yt, par):
    p, q = par[HEAD, 3], par[HEAD, 4]
    before, inv, w, qw = (BEFORE_W + k for k in range(4))
    us = []
    for k in range(NB):
        u = yt[k] + par[w, k] * yf[k]
        us.append(u if k == 0 else u + par[qw, k] * us[-1])
    fs = [None] * NB
    for k in reversed(range(NB)):
        g = yf[k]
        if k > 0:
            g = g + p * us[k - 1]
        if k < NB - 1:
            g = g + q * fs[k + 1]
        fs[k] = g * par[inv, k]
    zero = jnp.zeros_like(yf[0])
    ls = [zero] + [us[k - 1] + par[before, k] * fs[k] for k in range(1, NB)]
    return ls, fs[1:] + [zero]


def solve_wd(x, gw3, gd4):
    hi, lo = split(x)
    z = dot(gw3[:, : 2 * B], jnp.concatenate([hi, lo], axis=0)) + dot(gw3[:, 2 * B :], hi)
    z = jnp.concatenate([z[:, :D], z[:, D:]], axis=0)
    hi, lo = split(z)
    y = dot(jnp.concatenate([hi, lo], axis=1), gd4[...])
    return y[:, :D] + y[:, D:]


def edges_kernel(par, cr, cs, from_left, from_right, gw3, gd4, cols, out, e):
    c0, c1, c2 = par[HEAD, 0], par[HEAD, 1], par[HEAD, 2]
    row = iota((B, D), 0)
    lane = iota((B, D), 1)
    blank = jnp.zeros((B - 8, B), f32)
    for k in range(NB):
        spot = slice(k * B, (k + 1) * B)
        lc = jnp.concatenate([from_left[:, spot], blank], axis=0).T
        rc = jnp.concatenate([from_right[:, spot], blank], axis=0).T
        xs = []
        for j in range(2):
            x = cr[j, spot]
            up = pltpu.roll(x, 1, 0)
            up = jnp.where(row == 0, cr[j, k * B - 1 : k * B] if k > 0 else 0.0, up)
            down = pltpu.roll(x, B - 1, 0)
            down = jnp.where(row == B - 1, cr[j, (k + 1) * B : (k + 1) * B + 1] if k < NB - 1 else 0.0, down)
            lcol = lc if j == 0 else pltpu.roll(lc, D - 2, 1)
            left = jnp.where(lane == 0, lcol, pltpu.roll(x, 1, 1))
            right = jnp.where(lane == D - 1, pltpu.roll(rc, D - 2 if j == 0 else D - 4, 1), pltpu.roll(x, D - 1, 1))
            xs.append(cs[j, spot] + c0 * x + c1 * (up + down) + c2 * (left + right))
        y = solve_wd(jnp.concatenate(xs, axis=1), gw3, gd4)
        e[0, spot] = y[:B]
        e[1, spot] = y[B:]
    for j in range(2):
        ls, rs = chain_w(
            [e[j, k * B : k * B + 1] for k in range(NB)], [e[j, k * B + B - 1 : k * B + B] for k in range(NB)], par
        )
        for k in range(NB):
            spot = slice(k * B, (k + 1) * B)
            e[j, spot] = e[j, spot] + cols[0] * ls[k] + cols[1] * rs[k]
        for p in range(NP):
            out[p, j] = e[j, S * p : S * (p + 1)]


def field_kernel(par, rho, prev, nxt, sig, gw3, gd4, out, ew, e):
    i = pl.program_id(0)
    c0, c1, c2 = par[HEAD, 0], par[HEAD, 1], par[HEAD, 2]
    row = iota((B, D), 0)
    for h in range(H):
        x = rho[h]
        up = jnp.where(row == 0, jnp.where(i > 0, prev[h, 7:8, :], 0.0), pltpu.roll(x, 1, 0))
        down = jnp.where(row == B - 1, jnp.where(i < NB - 1, nxt[h, 0:1, :], 0.0), pltpu.roll(x, B - 1, 0))
        e[h] = sig[h] + c0 * x + c1 * (up + down) + c2 * (pltpu.roll(x, 1, 1) + pltpu.roll(x, D - 1, 1))

    def tile(j, _):
        at = pl.ds(pl.multiple_of(8 * j, 8), 8)
        z = []
        for h in range(H):
            v = par[MH, h] * e[h, at, :]
            z.append(v if h == 0 else v + par[CH, h] * z[-1])
        x = z[H - 1]
        e[H - 1, at, :] = x - 2.0 * rho[H - 1, at, :]
        for h in reversed(range(H - 1)):
            x = z[h] + par[CH, h] * x
            e[h, at, :] = x - 2.0 * rho[h, at, :]
        return 0

    lax.fori_loop(0, B // 8, tile, 0)
    for g in range(H // 2):
        y = solve_wd(jnp.concatenate([e[2 * g], e[2 * g + 1]], axis=1), gw3, gd4)
        for side in range(2):
            h = 2 * g + side
            part = y[side * B : (side + 1) * B]
            ew[0, 0, h : h + 1, :] = part[0:1]
            ew[0, 1, h : h + 1, :] = part[B - 1 : B]
            out[h] = part + rho[h]


def mend_kernel(par, base, ew, cols, out, qp, fix, packed):
    i = pl.program_id(0)

    @pl.when(i == 0)
    def _():
        ls, rs = chain_w([ew[k, 0] for k in range(NB)], [ew[k, 1] for k in range(NB)], par)
        for k in range(NB):
            fix[k, 0] = ls[k]
            fix[k, 1] = rs[k]

    lane = iota((B, D), 1)
    pack = jnp.zeros((B, D), f32)
    for h in range(H):
        v = base[h] + cols[0] * fix[i, 0, h : h + 1, :] + cols[1] * fix[i, 1, h : h + 1, :]
        out[h] = v
        pack = jnp.where((lane == 2 * h) | (lane == 2 * h + 1), pltpu.roll(v, 2 * h + 1, 1), pack)
    packed[...] = pack.T[: 2 * H]
    qp[:H] = packed[pl.ds(1, H, stride=2), :]
    qp[H:] = packed[pl.ds(0, H, stride=2), :]


def planes_kernel(par, qp, own, from_left, from_right, hmat, rows, wi, out, u):
    v = jnp.concatenate([from_left[H:] - own[H:], from_right[:H] - own[:H]], axis=0)
    v = jnp.dot(hmat[:, : 2 * H], v, precision=HIGHEST, preferred_element_type=f32)
    parts = []
    for k in range(NB):
        parts.append(
            lax.dot_general(
                v[:, k * B : (k + 1) * B], wi[0], (((1,), (1,)), ((), ())), precision=HIGHEST, preferred_element_type=f32
            )
        )
    ls, rs = chain_w([a[:, 0:1] for a in parts], [a[:, B - 1 : B] for a in parts], par)
    for k in range(NB):
        spot = slice(k * B, (k + 1) * B)
        u[:, spot] = 2.0 * (parts[k] + ls[k] * rows[0:1] + rs[k] * rows[1:2])
    p, q = par[HEAD, 7], par[HEAD, 8]
    ul, ur = u[:H], u[H:]
    out[:H] = qp[:H] - own[:H] + p * ul + q * ur
    out[H:] = qp[H:] - own[H:] + q * ul + p * ur


def solver_kernel(par, y, out, us):
    p, q = par[HEAD, 5], par[HEAD, 6]
    before, inv, w, qw = (BEFORE_H + k for k in range(4))
    u = y[0, 1] + par[w, 0] * y[0, 0]
    us[0] = u
    for k in range(1, NP):
        u = y[k, 1] + par[w, k] * y[k, 0] + par[qw, k] * u
        us[k] = u
    zero = jnp.zeros_like(u)
    out[NP - 1, 1] = zero
    f = zero
    for k in reversed(range(NP)):
        g = y[k, 0]
        if k > 0:
            g = g + p * us[k - 1]
        f = (g + q * f) * par[inv, k]
        if k > 0:
            out[k, 0] = us[k - 1] + par[before, k] * f
            out[k - 1, 1] = f
    out[0, 0] = zero


def corner_kernel(a, out, wide):
    lane = iota((S, D), 1)
    for p in range(NP):
        wide[S * p : S * (p + 1)] = jnp.where(lane < 2, pltpu.roll(a[p, 0], 1, 1), pltpu.roll(a[p, 1], 3, 1))
    for k in range(NB):
        out[:, k * B : (k + 1) * B] = wide[k * B : (k + 1) * B].T[:8]


def final_kernel(par, base, a, d0, d1, d2, d3, c0, c1, c2, c3, u, hcol, spread, out, tall):
    i = pl.program_id(0)

    @pl.when(i == 0)
    def _():
        ds, cs = (d0, d1, d2, d3), (c0, c1, c2, c3)
        sides = []
        for side in range(2):
            first, last = FROM + 2 * side, FROM + 2 * side + 1
            own = u[H * side : H * (side + 1)]
            for k in range(4):
                own = own + par[first, k] * ds[k][:H] + par[last, k] * ds[k][H:]
            gam = []
            for plane in range(2):
                g = 0.0
                for k in range(4):
                    t, f = cs[k][2 * plane : 2 * plane + 1], cs[k][2 * plane + 1 : 2 * plane + 2]
                    g = g + par[first, k] * f + par[last, k] * t
                gam.append(g)
            sides.append(own + hcol[:, 0:1] * gam[0] + hcol[:, 1:2] * gam[1])
        both = jnp.concatenate(sides + [jnp.zeros((D - 2 * H, W), f32)], axis=0)
        for k in range(NB):
            tall[k * B : (k + 1) * B] = both[:, k * B : (k + 1) * B].T

    at = pl.ds(pl.multiple_of(i * 4 * S, 4 * S), 4 * S)
    hi, lo = split(tall[at, : 2 * H])
    wide = dot(jnp.concatenate([hi, lo, hi], axis=1), spread[...])
    l = jnp.concatenate([a[p, 0] for p in range(4)], axis=0)
    r = jnp.concatenate([a[p, 1] for p in range(4)], axis=0)
    for h in range(H):
        out[h] = base[h] + wide[:, h * D : (h + 1) * D] + par[AH, h] * l + par[AH, H - 1 - h] * r


SMEM = pl.BlockSpec(memory_space=pltpu.SMEM)


def whole(*shape):
    return pl.BlockSpec(shape, lambda *_: (0,) * len(shape))


def shaped(*shape, dtype=f32):
    return jax.ShapeDtypeStruct(shape, dtype)


def cost(flops, bytes_accessed):
    return pl.CostEstimate(flops=flops, bytes_accessed=bytes_accessed, transcendentals=0)


def per_device(density, source, coupling, width_inverse, height_inverse, depth_inverse):
    slab = lax.axis_index("slab")
    slabs = lax.axis_size("slab")
    up = [(k, k + 1) for k in range(slabs - 1)]
    down = [(k + 1, k) for k in range(slabs - 1)]

    block = pl.BlockSpec((H, B, D), lambda i: (0, i, 0))
    pair = pl.BlockSpec((2, B, D), lambda i: (0, i, 0))
    line = pl.BlockSpec((2 * H, B), lambda i: (0, i))
    cr, cs, own, comb = pl.pallas_call(
        sums_kernel,
        grid=(NB,),
        in_specs=[SMEM, block, block],
        out_specs=[pair, pair, line, pl.BlockSpec((8, B), lambda i: (0, i))],
        out_shape=[shaped(2, W, D), shaped(2, W, D), shaped(2 * H, W), shaped(8, W)],
        scratch_shapes=[pltpu.VMEM((H, 8, 128), f32), pltpu.VMEM((2 * H, B), f32)],
        name="sums",
        cost_estimate=cost(10**7, 14 * 10**6),
    )(coupling, density, source)
    comb_left = lax.ppermute(comb, "slab", up)
    comb_right = lax.ppermute(comb, "slab", down)

    first_block = pl.BlockSpec((1, B, B), lambda *_: (0, 0, 0))
    par, cols, rows, gw3, gd4, spread, hmat, hcol = pl.pallas_call(
        tables_kernel,
        grid=(1,),
        in_specs=[SMEM, SMEM, first_block, first_block],
        out_specs=[
            whole(16, 128),
            whole(2, B, D),
            whole(8, 128),
            whole(B, 3 * B),
            whole(2 * D, 2 * D),
            whole(6 * H, H * D),
            whole(2 * H, 128),
            whole(H, 128),
        ],
        out_shape=[
            shaped(16, 128),
            shaped(2, B, D),
            shaped(8, 128),
            shaped(B, 3 * B, dtype=bf16),
            shaped(2 * D, 2 * D, dtype=bf16),
            shaped(6 * H, H * D, dtype=bf16),
            shaped(2 * H, 128),
            shaped(H, 128),
        ],
        name="tables",
        cost_estimate=cost(10**7, 10**6),
    )(coupling, slab.reshape(1), width_inverse, depth_inverse)

    edges = pl.pallas_call(
        edges_kernel,
        grid=(1,),
        in_specs=[SMEM, whole(2, W, D), whole(2, W, D), whole(8, W), whole(8, W), whole(B, 3 * B), whole(2 * D, 2 * D), whole(2, B, D)],
        out_specs=whole(NP, 2, S, D),
        out_shape=shaped(NP, 2, S, D),
        scratch_shapes=[pltpu.VMEM((2, W, D), f32)],
        name="edges",
        cost_estimate=cost(10**8, 3 * 10**6),
    )(par, cr, cs, comb_left, comb_right, gw3, gd4, cols)
    arrived = lax.all_to_all(edges, "pencil", 0, 0, tiled=True)

    own_left = lax.ppermute(own, "slab", up)
    own_right = lax.ppermute(own, "slab", down)
    raw, ew = pl.pallas_call(
        field_kernel,
        grid=(NB,),
        in_specs=[
            SMEM,
            block,
            pl.BlockSpec((H, 8, D), lambda i: (0, jnp.maximum(i * (B // 8) - 1, 0), 0)),
            pl.BlockSpec((H, 8, D), lambda i: (0, jnp.minimum((i + 1) * (B // 8), W // 8 - 1), 0)),
            block,
            whole(B, 3 * B),
            whole(2 * D, 2 * D),
        ],
        out_specs=[block, pl.BlockSpec((1, 2, H, D), lambda i: (i, 0, 0, 0))],
        out_shape=[shaped(H, W, D), shaped(NB, 2, H, D)],
        scratch_shapes=[pltpu.VMEM((H, B, D), f32)],
        name="field",
        cost_estimate=cost(4 * 10**9, 19 * 10**6),
    )(par, density, density, density, source, gw3, gd4)

    arrived, ew = lax.optimization_barrier((arrived, ew))
    solved = pl.pallas_call(
        solver_kernel,
        grid=(1,),
        in_specs=[SMEM, whole(NP, 2, S, D)],
        out_specs=whole(NP, 2, S, D),
        out_shape=shaped(NP, 2, S, D),
        scratch_shapes=[pltpu.VMEM((NP, S, D), f32)],
        name="solver",
        cost_estimate=cost(10**6, 2 * 10**6),
    )(par, arrived)
    outside = lax.all_to_all(solved, "pencil", 0, 0, tiled=True)

    base, qp = pl.pallas_call(
        mend_kernel,
        grid=(NB,),
        in_specs=[SMEM, block, whole(NB, 2, H, D), whole(2, B, D)],
        out_specs=[block, line],
        out_shape=[shaped(H, W, D), shaped(2 * H, W)],
        scratch_shapes=[pltpu.VMEM((NB, 2, H, D), f32), pltpu.VMEM((2 * H, B), f32)],
        input_output_aliases={1: 0},
        name="mend",
        cost_estimate=cost(10**9, 13 * 10**6),
    )(par, raw, ew, cols)
    planes, u = pl.pallas_call(
        planes_kernel,
        grid=(1,),
        in_specs=[SMEM, *[whole(2 * H, W)] * 4, whole(2 * H, 128), whole(8, 128), first_block],
        out_specs=[whole(2 * H, W)] * 2,
        out_shape=[shaped(2 * H, W)] * 2,
        name="planes",
        cost_estimate=cost(10**8, 10**6),
    )(par, qp, own, own_left, own_right, hmat, rows, width_inverse)

    def turned(value):
        return [value] + [
            lax.ppermute(value, "slab", [(k, (k + d) % slabs) for k in range(slabs)]) for d in range(1, slabs)
        ]

    planes_all = turned(planes)
    corners = pl.pallas_call(
        corner_kernel,
        grid=(1,),
        in_specs=[whole(NP, 2, S, D)],
        out_specs=whole(8, W),
        out_shape=shaped(8, W),
        scratch_shapes=[pltpu.VMEM((W, D), f32)],
        name="corner",
        cost_estimate=cost(10**6, 10**6),
    )(outside)
    corners_all = turned(corners)
    return pl.pallas_call(
        final_kernel,
        grid=(NP // 4,),
        in_specs=[
            SMEM,
            pl.BlockSpec((H, 4 * S, D), lambda i: (0, i, 0)),
            pl.BlockSpec((4, 2, S, D), lambda i: (i, 0, 0, 0)),
            *[whole(2 * H, W)] * 4,
            *[whole(8, W)] * 4,
            whole(2 * H, W),
            whole(H, 128),
            whole(6 * H, H * D),
        ],
        out_specs=pl.BlockSpec((H, 4 * S, D), lambda i: (0, i, 0)),
        out_shape=shaped(H, W, D),
        scratch_shapes=[pltpu.VMEM((W, D), f32)],
        name="final",
        cost_estimate=cost(10**9, 13 * 10**6),
    )(par, base, outside, *planes_all, *corners_all, u, hcol, spread)


def solution(mesh):
    in_specs = (P("pencil", None, "slab"), P("pencil", None, "slab"), P(), P(), P(), P())
    out_specs = P("pencil", None, "slab")
    return jax.shard_map(per_device, mesh=mesh, in_specs=in_specs, out_specs=out_specs, check_vma=False)
```

```python
import jax
import jax.numpy as jnp
from jax import lax
from jax.experimental import pallas as pl
from jax.experimental.pallas import tpu as pltpu
from jax.sharding import PartitionSpec as P

H, W, D = 16, 768, 128
B = 128
NB = W // B
NP = 32
S = W // NP
T = 16
f32 = jnp.float32
bf16 = jnp.bfloat16
HIGHEST = lax.Precision.HIGHEST


def log_decay(s):
    return jnp.log(2.0 * s / (1.0 + 2.0 * s + jnp.sqrt(1.0 + 4.0 * s)))


def pivots(log_r, length):
    return (
        jnp.exp(log_r)
        * (1.0 - jnp.exp(log_r * (2.0 * length)))
        / (1.0 - jnp.exp(log_r * (2.0 * length + 2.0)))
    )


def influence(log_r, m, i):
    return (
        jnp.exp(log_r * (i + 1.0))
        * (1.0 - jnp.exp(log_r * (2.0 * (m - i))))
        / (1.0 - jnp.exp(log_r * (2.0 * m + 2.0)))
    )


def green(s, log_r, n, i, j):
    low, high = jnp.minimum(i, j), jnp.maximum(i, j)
    return (
        jnp.exp(log_r * (high - low))
        * (1.0 - jnp.exp(log_r * (2.0 * low + 2.0)))
        * (1.0 - jnp.exp(log_r * (2.0 * (n - high))))
        / (jnp.sqrt(1.0 + 4.0 * s) * (1.0 - jnp.exp(log_r * (2.0 * n + 2.0))))
    )


def split(x):
    hi = x.astype(bf16)
    return hi, (x - hi.astype(f32)).astype(bf16)


def dot(a, b):
    return lax.dot_general(a, b, (((1,), (0,)), ((), ())), preferred_element_type=f32)


def iota(shape, dim):
    return lax.broadcasted_iota(jnp.int32, shape, dim)


HEAD, BEFORE_H, BEFORE_W, AH, CH, MH, FROM = 0, 1, 5, 9, 10, 11, 12


def tables_kernel(cpl, slab, wi, di, par, cols, rows, gw3, gd4, spread, hmat, hcol, gwf):
    row = (1, 128)
    sw, sh, sd = (jnp.full(row, cpl[k], f32) for k in range(3))
    lw, lh, ld = log_decay(sw), log_decay(sh), log_decay(sd)
    lane = iota(row, 1)
    k = lane.astype(f32)
    heads = [2.0 - 4.0 * sw - 4.0 * sd, 2.0 * sw, 2.0 * sd]
    for log_r, m in ((lw, float(B)), (lh, float(H)), (ld, float(D))):
        heads += [influence(log_r, m, 0.0), influence(log_r, m, m - 1.0)]
    middle = pivots(lh, float(H // 2))
    heads.append(1.0 / (1.0 - middle * middle))
    head = jnp.zeros(row, f32)
    for at, v in enumerate(heads):
        head = jnp.where(lane == at, v, head)
    par[HEAD : HEAD + 1] = head
    for at, log_r, m, p, q in ((BEFORE_H, lh, float(H), heads[5], heads[6]), (BEFORE_W, lw, float(B), heads[3], heads[4])):
        before = pivots(log_r, m * k)
        inv = 1.0 / (1.0 - p * before)
        w = q * before * inv
        for n, v in enumerate((before, inv, w, q + w * p)):
            par[at + n : at + n + 1] = v
    kc = jnp.minimum(k, H - 1.0)
    ch = pivots(lh, kc + 1.0)
    par[AH : AH + 1] = influence(lh, float(H), kc)
    par[CH : CH + 1] = ch
    par[MH : MH + 1] = ch / sh
    me = slab[0]
    other = lax.bitwise_and(me - lane, 3)
    of, mf = other.astype(f32), jnp.full(row, me, jnp.int32).astype(f32)
    n = float(4 * D)
    for side, (where, beside, inside) in enumerate(
        ((D * mf - 1.0, me - 1, me > 0), (D * mf + D, me + 1, me < 3))
    ):
        spot = jnp.clip(where, 0.0, n - 1.0)
        first = jnp.where(other >= 1, sd * green(sd, ld, n, spot, jnp.maximum(D * of - 1.0, 0.0)), 0.0)
        last = jnp.where(other <= 2, sd * green(sd, ld, n, spot, jnp.minimum(D * of + D, n - 1.0)), 0.0)
        same = jnp.where(other == beside, 1.0, 0.0)
        if side == 0:
            last = last + same
        else:
            first = first + same
        par[FROM + 2 * side : FROM + 2 * side + 1] = jnp.where(inside, first, 0.0)
        par[FROM + 2 * side + 1 : FROM + 2 * side + 2] = jnp.where(inside, last, 0.0)
    tall = iota((B, D), 0).astype(f32)
    lww = jnp.broadcast_to(lw, (B, D))
    cols[0] = influence(lww, float(B), tall)
    cols[1] = influence(lww, float(B), B - 1.0 - tall)
    rows[0:1] = influence(lw, float(B), k)
    rows[1:2] = influence(lw, float(B), B - 1.0 - k)
    gwf[...] = wi[0]
    hi, lo = split(wi[0])
    gw3[:, :B] = hi
    gw3[:, B : 2 * B] = hi
    gw3[:, 2 * B :] = lo
    hi, lo = split(di[0].T)
    gd4[:D, :D] = hi
    gd4[:D, D:] = lo
    gd4[D:, :D] = hi
    gd4[D:, D:] = jnp.zeros((D, D), bf16)
    ad, bd = influence(ld, float(D), k), influence(ld, float(D), D - 1.0 - k)
    line = iota((2 * H, D), 0)
    for h in range(H):
        v = jnp.where(line == h, ad, jnp.where(line == H + h, bd, 0.0))
        hi, lo = split(v)
        at = slice(h * D, (h + 1) * D)
        spread[: 2 * H, at] = hi
        spread[2 * H : 4 * H, at] = hi
        spread[4 * H :, at] = lo
    a = iota((2 * H, 128), 0)
    b = iota((2 * H, 128), 1)
    af = lax.bitwise_and(a, H - 1).astype(f32)
    bfl = lax.bitwise_and(b, H - 1).astype(f32)
    wide_h = jnp.broadcast_to(lh, (2 * H, 128))
    g = green(jnp.broadcast_to(sh, (2 * H, 128)), wide_h, float(H), af, bfl)
    hmat[...] = jnp.where((b < 2 * H) & (lax.shift_right_logical(a, 4) == lax.shift_right_logical(b, 4)), g, 0.0)
    c = iota((H, 128), 0).astype(f32)
    ln = iota((H, 128), 1)
    hcol[...] = influence(jnp.broadcast_to(lh, (H, 128)), float(H), jnp.where(ln == 0, c, H - 1.0 - c))


def sums_kernel(cpl, rho, sig, cr, cs, halo, rv, sv, coef, packed, sems):
    def parts(i):
        at = pl.ds(pl.multiple_of(i * B, B), B)
        return (
            pltpu.make_async_copy(rho.at[:, at, :], rv.at[:, at, :], sems.at[0, i]),
            pltpu.make_async_copy(sig.at[:, at, :], sv.at[:, at, :], sems.at[1, i]),
        )

    for i in range(NB):
        for part in parts(i):
            part.start()
    sh = jnp.full((8, 128), cpl[1], f32)
    lh = log_decay(sh)
    for h in range(H):
        coef[h] = influence(lh, float(H), float(h)) / sh

    R = 32
    lane = iota((R, D), 1)

    def block(i, _):
        for part in parts(i):
            part.wait()
        packs, combs = [], []
        for t in range(B // R):
            at = pl.ds(pl.multiple_of(i * B + t * R, R), R)
            fr = jnp.zeros((R, D), f32)
            tr, fs, ts, pack = fr, fr, fr, fr
            for h in range(H):
                x, y = rv[h, at, :], sv[h, at, :]
                cf = jnp.broadcast_to(coef[h, 0:1, :], (R, D))
                ct = jnp.broadcast_to(coef[H - 1 - h, 0:1, :], (R, D))
                fr, tr, fs, ts = fr + cf * x, tr + ct * x, fs + cf * y, ts + ct * y
                pack = jnp.where((lane == 2 * h) | (lane == 2 * h + 1), pltpu.roll(x, 2 * h + 1, 1), pack)
            cr[0, at, :], cr[1, at, :], cs[0, at, :], cs[1, at, :] = fr, tr, fs, ts
            packs.append(pack)
            combs.append(jnp.where(lane < 2, pltpu.roll(fr, 1, 1), pltpu.roll(tr, 3, 1)))
        at = pl.ds(pl.multiple_of(i * B, B), B)
        packed[...] = jnp.concatenate(packs, axis=0).T[: 2 * H]
        halo[:H, at] = packed[pl.ds(1, H, stride=2), :]
        halo[H : 2 * H, at] = packed[pl.ds(0, H, stride=2), :]
        halo[2 * H :, at] = jnp.concatenate(combs, axis=0).T[:8]
        return 0

    lax.fori_loop(0, NB, block, 0)


def chain_w(yf, yt, par):
    p, q = par[HEAD, 3], par[HEAD, 4]
    before, inv, w, qw = (BEFORE_W + k for k in range(4))
    us = []
    for k in range(NB):
        u = yt[k] + par[w, k] * yf[k]
        us.append(u if k == 0 else u + par[qw, k] * us[-1])
    fs = [None] * NB
    for k in reversed(range(NB)):
        g = yf[k]
        if k > 0:
            g = g + p * us[k - 1]
        if k < NB - 1:
            g = g + q * fs[k + 1]
        fs[k] = g * par[inv, k]
    zero = jnp.zeros_like(yf[0])
    ls = [zero] + [us[k - 1] + par[before, k] * fs[k] for k in range(1, NB)]
    return ls, fs[1:] + [zero]


def solve_wd(x, gw3, gd4):
    hi, lo = split(x)
    z = dot(gw3[:, : 2 * B], jnp.concatenate([hi, lo], axis=0)) + dot(gw3[:, 2 * B :], hi)
    z = jnp.concatenate([z[:, :D], z[:, D:]], axis=0)
    hi, lo = split(z)
    y = dot(jnp.concatenate([hi, lo], axis=1), gd4[...])
    return y[:, :D] + y[:, D:]


def edges_kernel(par, cr, cs, from_left, from_right, gw3, gd4, cols, out, e):
    c0, c1, c2 = par[HEAD, 0], par[HEAD, 1], par[HEAD, 2]
    row = iota((B, D), 0)
    lane = iota((B, D), 1)
    blank = jnp.zeros((B - 8, B), f32)
    for k in range(NB):
        spot = slice(k * B, (k + 1) * B)
        lc = jnp.concatenate([from_left[2 * H :, spot], blank], axis=0).T
        rc = jnp.concatenate([from_right[2 * H :, spot], blank], axis=0).T
        xs = []
        for j in range(2):
            x = cr[j, spot]
            up = pltpu.roll(x, 1, 0)
            up = jnp.where(row == 0, cr[j, k * B - 1 : k * B] if k > 0 else 0.0, up)
            down = pltpu.roll(x, B - 1, 0)
            down = jnp.where(row == B - 1, cr[j, (k + 1) * B : (k + 1) * B + 1] if k < NB - 1 else 0.0, down)
            lcol = lc if j == 0 else pltpu.roll(lc, D - 2, 1)
            left = jnp.where(lane == 0, lcol, pltpu.roll(x, 1, 1))
            right = jnp.where(lane == D - 1, pltpu.roll(rc, D - 2 if j == 0 else D - 4, 1), pltpu.roll(x, D - 1, 1))
            xs.append(cs[j, spot] + c0 * x + c1 * (up + down) + c2 * (left + right))
        y = solve_wd(jnp.concatenate(xs, axis=1), gw3, gd4)
        e[0, spot] = y[:B]
        e[1, spot] = y[B:]
    for j in range(2):
        ls, rs = chain_w(
            [e[j, k * B : k * B + 1] for k in range(NB)], [e[j, k * B + B - 1 : k * B + B] for k in range(NB)], par
        )
        for k in range(NB):
            spot = slice(k * B, (k + 1) * B)
            e[j, spot] = e[j, spot] + cols[0] * ls[k] + cols[1] * rs[k]
        for p in range(NP):
            out[p, j] = e[j, S * p : S * (p + 1)]


def field_kernel(par, rho, sig, gw3, gd4, raw, ew, qp, rv, out, packed, sems):
    sv = out

    def parts(i):
        at = pl.ds(pl.multiple_of(i * B, B), B)
        return (
            pltpu.make_async_copy(rho.at[:, at, :], rv.at[:, at, :], sems.at[0, i]),
            pltpu.make_async_copy(sig.at[:, at, :], out.at[:, at, :], sems.at[1, i]),
        )

    def send(i):
        at = pl.ds(pl.multiple_of(i * B, B), B)
        return pltpu.make_async_copy(out.at[:, at, :], raw.at[:, at, :], sems.at[2, i])

    for i in range(NB):
        for part in parts(i):
            part.start()
    for part in parts(0):
        part.wait()
    c0, c1, c2 = par[HEAD, 0], par[HEAD, 1], par[HEAD, 2]
    row = iota((B, D), 0)
    half = H // 2
    meet = par[HEAD, 9]

    def block(i, _):
        @pl.when(i < NB - 1)
        def _():
            for part in parts(jnp.minimum(i + 1, NB - 1)):
                part.wait()

        here = pl.ds(pl.multiple_of(i * B, B), B)
        before = pl.ds(pl.multiple_of(jnp.maximum(i * B - 8, 0), 8), 8)
        after = pl.ds(pl.multiple_of(jnp.minimum(i * B + B, W - 8), 8), 8)
        for h in range(H):
            x = rv[h, here, :]
            first = jnp.where(i > 0, rv[h, before, :][7:8], 0.0)
            last = jnp.where(i < NB - 1, rv[h, after, :][0:1], 0.0)
            up = jnp.where(row == 0, first, pltpu.roll(x, 1, 0))
            down = jnp.where(row == B - 1, last, pltpu.roll(x, B - 1, 0))
            out[h, here, :] = (
                sv[h, here, :] + c0 * x + c1 * (up + down) + c2 * (pltpu.roll(x, 1, 1) + pltpu.roll(x, D - 1, 1))
            )

        def tile(j, _):
            at = pl.ds(pl.multiple_of(i * B + T * j, T), T)
            top, bottom = [None] * half, [None] * half
            for h in range(half):
                m, c = par[MH, h], par[CH, h]
                a, b = m * out[h, at, :], m * out[H - 1 - h, at, :]
                top[h] = a if h == 0 else a + c * top[h - 1]
                bottom[h] = b if h == 0 else b + c * bottom[h - 1]
            c = par[CH, half - 1]
            x = (top[half - 1] + c * bottom[half - 1]) * meet
            y = bottom[half - 1] + c * x
            for h in reversed(range(half)):
                if h < half - 1:
                    c = par[CH, h]
                    x, y = top[h] + c * x, bottom[h] + c * y
                out[h, at, :] = x - 2.0 * rv[h, at, :]
                out[H - 1 - h, at, :] = y - 2.0 * rv[H - 1 - h, at, :]
            return 0

        lax.fori_loop(0, B // T, tile, 0)
        lane = iota((B, D), 1)
        pack = jnp.zeros((B, D), f32)
        for g in range(H // 2):
            y = solve_wd(jnp.concatenate([out[2 * g, here, :], out[2 * g + 1, here, :]], axis=1), gw3, gd4)
            for side in range(2):
                h = 2 * g + side
                part = y[side * B : (side + 1) * B]
                ew[i, 0, h : h + 1, :] = part[0:1]
                ew[i, 1, h : h + 1, :] = part[B - 1 : B]
                out[h, here, :] = part + rv[h, here, :]
                pack = jnp.where((lane == 2 * h) | (lane == 2 * h + 1), pltpu.roll(part, 2 * h + 1, 1), pack)
        packed[...] = pack.T[: 2 * H]
        qp[:H, here] = packed[pl.ds(1, H, stride=2), :]
        qp[H:, here] = packed[pl.ds(0, H, stride=2), :]
        send(i).start()
        return 0

    lax.fori_loop(0, NB, block, 0)
    for i in range(NB):
        send(i).wait()


def planes_kernel(par, ew, qp, own, from_left, from_right, hmat, rows, gwf, planes, u, fix):
    ls, rs = chain_w([ew[k, 0] for k in range(NB)], [ew[k, 1] for k in range(NB)], par)
    for k in range(NB):
        fix[k, 0] = ls[k]
        fix[k, 1] = rs[k]
    v = jnp.concatenate([from_left[H : 2 * H] - own[H : 2 * H], from_right[:H] - own[:H]], axis=0)
    v = jnp.dot(hmat[:, : 2 * H], v, precision=HIGHEST, preferred_element_type=f32)
    parts = []
    for k in range(NB):
        spot = slice(k * B, (k + 1) * B)
        solved = lax.dot_general(
            v[:, spot], gwf[...], (((1,), (1,)), ((), ())), precision=HIGHEST, preferred_element_type=f32
        )
        parts.append(jnp.concatenate([2.0 * solved, qp[:, spot]], axis=0))
    ls, rs = chain_w([a[:, 0:1] for a in parts], [a[:, B - 1 : B] for a in parts], par)
    p, q = par[HEAD, 7], par[HEAD, 8]
    for k in range(NB):
        spot = slice(k * B, (k + 1) * B)
        both = parts[k] + ls[k] * rows[0:1] + rs[k] * rows[1:2]
        ul, ur = both[:H], both[H : 2 * H]
        u[:, spot] = both[: 2 * H]
        planes[:H, spot] = both[2 * H : 3 * H] + p * ul + q * ur
        planes[H:, spot] = both[3 * H :] + q * ul + p * ur


def solver_kernel(par, y, out, us):
    p, q = par[HEAD, 5], par[HEAD, 6]
    before, inv, w, qw = (BEFORE_H + k for k in range(4))
    u = y[0, 1] + par[w, 0] * y[0, 0]
    us[0] = u
    for k in range(1, NP):
        u = y[k, 1] + par[w, k] * y[k, 0] + par[qw, k] * u
        us[k] = u
    zero = jnp.zeros_like(u)
    out[NP - 1, 1] = zero
    f = zero
    for k in reversed(range(NP)):
        g = y[k, 0]
        if k > 0:
            g = g + p * us[k - 1]
        f = (g + q * f) * par[inv, k]
        if k > 0:
            out[k, 0] = us[k - 1] + par[before, k] * f
            out[k - 1, 1] = f
    out[0, 0] = zero


def corner_kernel(a, out, wide):
    lane = iota((S, D), 1)
    for p in range(NP):
        wide[S * p : S * (p + 1)] = jnp.where(lane < 2, pltpu.roll(a[p, 0], 1, 1), pltpu.roll(a[p, 1], 3, 1))
    for k in range(NB):
        out[:, k * B : (k + 1) * B] = wide[k * B : (k + 1) * B].T[:8]


def nearly_kernel(par, raw, a, fix, cols, out, lr, sems):
    def part(i):
        at = pl.ds(pl.multiple_of(i * B, B), B)
        return pltpu.make_async_copy(raw.at[:, at, :], out.at[:, at, :], sems.at[i])

    for i in range(NB):
        part(i).start()
    for p in range(NP):
        for j in range(2):
            lr[j, S * p : S * (p + 1)] = a[p, j]
    R = 32

    def block(i, _):
        part(i).wait()
        for t in range(B // R):
            at = pl.ds(pl.multiple_of(i * B + t * R, R), R)
            ca, cb = cols[0, t * R : (t + 1) * R], cols[1, t * R : (t + 1) * R]
            l, r = lr[0, at, :], lr[1, at, :]
            for h in range(H):
                v = ca * fix[i, 0, h : h + 1, :] + cb * fix[i, 1, h : h + 1, :]
                out[h, at, :] = out[h, at, :] + v + (par[AH, h] * l + par[AH, H - 1 - h] * r)
        return 0

    lax.fori_loop(0, NB, block, 0)


def final_kernel(par, base, d0, d1, d2, d3, c0, c1, c2, c3, u, hcol, spread, out, tall, buf, sems):
    ds, cs = (d0, d1, d2, d3), (c0, c1, c2, c3)
    sides = []
    for side in range(2):
        first, last = FROM + 2 * side, FROM + 2 * side + 1
        own = u[H * side : H * (side + 1)]
        for k in range(4):
            own = own + par[first, k] * ds[k][:H] + par[last, k] * ds[k][H:]
        gam = []
        for plane in range(2):
            g = 0.0
            for k in range(4):
                t, f = cs[k][2 * plane : 2 * plane + 1], cs[k][2 * plane + 1 : 2 * plane + 2]
                g = g + par[first, k] * f + par[last, k] * t
            gam.append(g)
        sides.append(own + hcol[:, 0:1] * gam[0] + hcol[:, 1:2] * gam[1])
    both = jnp.concatenate(sides + [jnp.zeros((D - 2 * H, W), f32)], axis=0)
    for k in range(NB):
        tall[k * B : (k + 1) * B] = both[:, k * B : (k + 1) * B].T

    def send(i):
        at = pl.ds(pl.multiple_of(i * B, B), B)
        return pltpu.make_async_copy(buf.at[:, at, :], out.at[:, at, :], sems.at[i])

    def block(i, _):
        at = pl.ds(pl.multiple_of(i * B, B), B)
        hi, lo = split(tall[at, : 2 * H])
        wide = dot(jnp.concatenate([hi, lo, hi], axis=1), spread[...])
        for h in range(H):
            buf[h, at, :] = base[h, at, :] + wide[:, h * D : (h + 1) * D]
        send(i).start()
        return 0

    lax.fori_loop(0, NB, block, 0)
    for i in range(NB):
        send(i).wait()


SMEM = pl.BlockSpec(memory_space=pltpu.SMEM)
VMEM = pl.BlockSpec(memory_space=pltpu.VMEM)
HBM = pl.BlockSpec(memory_space=pltpu.HBM)


def limit(mib):
    return pltpu.CompilerParams(vmem_limit_bytes=mib * 2**20)


def held(*shape, dtype=f32):
    return pltpu.VMEM(shape, dtype)


def near(x):
    return pltpu.with_memory_space_constraint(x, pltpu.VMEM)


def far(x):
    return pltpu.with_memory_space_constraint(x, pltpu.HBM)


def cost(flops, bytes_accessed):
    return pl.CostEstimate(flops=flops, bytes_accessed=bytes_accessed, transcendentals=0)


def per_device(density, source, coupling, width_inverse, height_inverse, depth_inverse):
    slab = lax.axis_index("slab")
    slabs = lax.axis_size("slab")
    up = [(k, k + 1) for k in range(slabs - 1)]
    down = [(k + 1, k) for k in range(slabs - 1)]
    grid = [pltpu.VMEM((H, W, D), f32)]

    cr, cs, halo = pl.pallas_call(
        sums_kernel,
        in_specs=[SMEM, HBM, HBM],
        out_specs=[VMEM] * 3,
        out_shape=[held(2, W, D), held(2, W, D), held(2 * H + 8, W)],
        scratch_shapes=grid * 2
        + [pltpu.VMEM((H, 8, 128), f32), pltpu.VMEM((2 * H, B), f32), pltpu.SemaphoreType.DMA((2, NB))],
        compiler_params=limit(24),
        name="sums",
        cost_estimate=cost(10**7, 14 * 10**6),
    )(coupling, far(density), far(source))
    halo_left = lax.ppermute(halo, "slab", up)
    halo_right = lax.ppermute(halo, "slab", down)

    first = pl.BlockSpec((1, B, B), lambda *_: (0, 0, 0))
    shapes = [
        ((16, 128), f32),
        ((2, B, D), f32),
        ((8, 128), f32),
        ((B, 3 * B), bf16),
        ((2 * D, 2 * D), bf16),
        ((6 * H, H * D), bf16),
        ((2 * H, 128), f32),
        ((H, 128), f32),
        ((B, B), f32),
    ]
    par, cols, rows, gw3, gd4, spread, hmat, hcol, gwf = pl.pallas_call(
        tables_kernel,
        grid=(1,),
        in_specs=[SMEM, SMEM, first, first],
        out_specs=[pl.BlockSpec(shape, lambda *_, n=len(shape): (0,) * n) for shape, _ in shapes],
        out_shape=[jax.ShapeDtypeStruct(*shapes[0])] + [held(*shape, dtype=kind) for shape, kind in shapes[1:]],
        compiler_params=limit(8),
        name="tables",
        cost_estimate=cost(10**7, 10**6),
    )(coupling, slab.reshape(1), width_inverse, depth_inverse)

    edges = pl.pallas_call(
        edges_kernel,
        in_specs=[SMEM] + [VMEM] * 7,
        out_specs=VMEM,
        out_shape=held(NP, 2, S, D),
        scratch_shapes=[pltpu.VMEM((2, W, D), f32)],
        compiler_params=limit(8),
        name="edges",
        cost_estimate=cost(10**8, 3 * 10**6),
    )(par, near(cr), near(cs), near(halo_left), near(halo_right), near(gw3), near(gd4), near(cols))
    arrived = lax.all_to_all(edges, "pencil", 0, 0, tiled=True)

    raw, ew, qp = pl.pallas_call(
        field_kernel,
        in_specs=[SMEM, HBM, HBM, VMEM, VMEM],
        out_specs=[HBM, VMEM, VMEM],
        out_shape=[pltpu.HBM((H, W, D), f32), held(NB, 2, H, D), held(2 * H, W)],
        scratch_shapes=grid * 2 + [pltpu.VMEM((2 * H, B), f32), pltpu.SemaphoreType.DMA((3, NB))],
        compiler_params=limit(24),
        name="field",
        cost_estimate=cost(4 * 10**9, 19 * 10**6),
    )(par, far(density), far(source), near(gw3), near(gd4))

    arrived, ew = lax.optimization_barrier((arrived, ew))
    solved = pl.pallas_call(
        solver_kernel,
        in_specs=[SMEM, VMEM],
        out_specs=VMEM,
        out_shape=held(NP, 2, S, D),
        scratch_shapes=[pltpu.VMEM((NP, S, D), f32)],
        compiler_params=limit(8),
        name="solver",
        cost_estimate=cost(10**6, 2 * 10**6),
    )(par, near(arrived))
    outside = lax.all_to_all(solved, "pencil", 0, 0, tiled=True)

    planes, u, fix = pl.pallas_call(
        planes_kernel,
        in_specs=[SMEM] + [VMEM] * 8,
        out_specs=[VMEM] * 3,
        out_shape=[held(2 * H, W), held(2 * H, W), held(NB, 2, H, D)],
        compiler_params=limit(8),
        name="planes",
        cost_estimate=cost(10**8, 10**6),
    )(par, near(ew), near(qp), near(halo), near(halo_left), near(halo_right), near(hmat), near(rows), near(gwf))

    def turned(value):
        return [value] + [
            lax.ppermute(value, "slab", [(k, (k + d) % slabs) for k in range(slabs)]) for d in range(1, slabs)
        ]

    planes_all = turned(planes)
    outside = near(outside)
    corners = pl.pallas_call(
        corner_kernel,
        in_specs=[VMEM],
        out_specs=VMEM,
        out_shape=held(8, W),
        scratch_shapes=[pltpu.VMEM((W, D), f32)],
        compiler_params=limit(8),
        name="corner",
        cost_estimate=cost(10**6, 10**6),
    )(outside)
    corners_all = turned(corners)
    base = pl.pallas_call(
        nearly_kernel,
        in_specs=[SMEM, HBM] + [VMEM] * 3,
        out_specs=VMEM,
        out_shape=held(H, W, D),
        scratch_shapes=[pltpu.VMEM((2, W, D), f32), pltpu.SemaphoreType.DMA((NB,))],
        compiler_params=limit(8),
        name="nearly",
        cost_estimate=cost(10**8, 7 * 10**6),
    )(par, far(raw), outside, near(fix), near(cols))
    return pl.pallas_call(
        final_kernel,
        in_specs=[SMEM] + [VMEM] * 12,
        out_specs=HBM,
        out_shape=pltpu.HBM((H, W, D), f32),
        scratch_shapes=[pltpu.VMEM((W, D), f32), *grid, pltpu.SemaphoreType.DMA((NB,))],
        compiler_params=limit(16),
        name="final",
        cost_estimate=cost(10**9, 13 * 10**6),
    )(par, near(base), *[near(v) for v in planes_all], *[near(v) for v in corners_all], near(u), near(hcol), near(spread))


def solution(mesh):
    in_specs = (P("pencil", None, "slab"), P("pencil", None, "slab"), P(), P(), P(), P())
    out_specs = P("pencil", None, "slab")
    return jax.shard_map(per_device, mesh=mesh, in_specs=in_specs, out_specs=out_specs, check_vma=False)
```

```python
from functools import partial

import jax
import jax.numpy as jnp
from jax import lax
from jax.experimental import pallas as pl
from jax.experimental.pallas import tpu as pltpu
from jax.sharding import PartitionSpec as P

H, W, D = 16, 768, 128
B = 128
NB = W // B
NP = 32
S = W // NP
T = 16
HALF = 3
f32 = jnp.float32
bf16 = jnp.bfloat16
HIGHEST = lax.Precision.HIGHEST


def log_decay(s):
    return jnp.log(2.0 * s / (1.0 + 2.0 * s + jnp.sqrt(1.0 + 4.0 * s)))


def pivots(log_r, length):
    return (
        jnp.exp(log_r)
        * (1.0 - jnp.exp(log_r * (2.0 * length)))
        / (1.0 - jnp.exp(log_r * (2.0 * length + 2.0)))
    )


def influence(log_r, m, i):
    return (
        jnp.exp(log_r * (i + 1.0))
        * (1.0 - jnp.exp(log_r * (2.0 * (m - i))))
        / (1.0 - jnp.exp(log_r * (2.0 * m + 2.0)))
    )


def green(s, log_r, n, i, j):
    low, high = jnp.minimum(i, j), jnp.maximum(i, j)
    return (
        jnp.exp(log_r * (high - low))
        * (1.0 - jnp.exp(log_r * (2.0 * low + 2.0)))
        * (1.0 - jnp.exp(log_r * (2.0 * (n - high))))
        / (jnp.sqrt(1.0 + 4.0 * s) * (1.0 - jnp.exp(log_r * (2.0 * n + 2.0))))
    )


def split(x):
    hi = x.astype(bf16)
    return hi, (x - hi.astype(f32)).astype(bf16)


def dot(a, b):
    return lax.dot_general(a, b, (((1,), (0,)), ((), ())), preferred_element_type=f32)


def iota(shape, dim):
    return lax.broadcasted_iota(jnp.int32, shape, dim)


HEAD, BEFORE_H, BEFORE_W, AH, CH, MH, PAIR = 0, 1, 5, 9, 10, 11, 12


def tables_kernel(cpl, slab, wi, di, par, cols, rows, gw3, gd4, spread, hmat, hcol, gwf, colm):
    row = (1, 128)
    sw, sh, sd = (jnp.full(row, cpl[k], f32) for k in range(3))
    lw, lh, ld = log_decay(sw), log_decay(sh), log_decay(sd)
    lane = iota(row, 1)
    k = lane.astype(f32)
    heads = [2.0 - 4.0 * sw - 4.0 * sd, 2.0 * sw, 2.0 * sd]
    for log_r, m in ((lw, float(B)), (lh, float(H)), (ld, float(D))):
        heads += [influence(log_r, m, 0.0), influence(log_r, m, m - 1.0)]
    middle = pivots(lh, float(H // 2))
    heads.append(1.0 / (1.0 - middle * middle))
    p, q = heads[7], heads[8]
    i1 = 1.0 / (1.0 - p * p)
    v = p + p * q * q * i1
    i2 = 1.0 / (1.0 - v * v)
    heads += [i2, i2 * v]
    one, none = jnp.ones(row, f32), jnp.zeros(row, f32)
    by_slab = (
        ((none, q * i1, q * i1 * p, one, none), (none,) * 5, (none, p * i1, i1, none, q * i1)),
        ((q * i1 * p, one, none, q * i1, none), (p * i1, none, none, i1, p * q * i1), (none,) * 4 + (one,)),
        ((one, q * i1 * p, q * i1, none, none), (none,) * 4 + (one,), (none, p * i1, i1, none, p * q * i1)),
        ((q * i1, none, one, q * i1 * p, none), (p * i1, none, none, i1, q * i1), (none,) * 5),
    )
    mine = jnp.full(row, slab[0], jnp.int32)
    for line in range(3):
        total = none
        for at in range(4):
            for n, value in enumerate(by_slab[at][line]):
                total = jnp.where((mine == at) & (lane == n), value, total)
        par[PAIR + line : PAIR + line + 1] = total
    head = jnp.zeros(row, f32)
    for at, v in enumerate(heads):
        head = jnp.where(lane == at, v, head)
    par[HEAD : HEAD + 1] = head
    for at, log_r, m, p, q in ((BEFORE_H, lh, float(H), heads[5], heads[6]), (BEFORE_W, lw, float(B), heads[3], heads[4])):
        before = pivots(log_r, m * k)
        inv = 1.0 / (1.0 - p * before)
        w = q * before * inv
        for n, v in enumerate((before, inv, w, q + w * p)):
            par[at + n : at + n + 1] = v
    kc = jnp.minimum(k, H - 1.0)
    ch = pivots(lh, kc + 1.0)
    par[AH : AH + 1] = influence(lh, float(H), kc)
    par[CH : CH + 1] = ch
    par[MH : MH + 1] = ch / sh
    tall = iota((B, D), 0).astype(f32)
    lww = jnp.broadcast_to(lw, (B, D))
    cols[0] = influence(lww, float(B), tall)
    cols[1] = influence(lww, float(B), B - 1.0 - tall)
    ca, cb = cols[0], cols[1]
    ca_hi, cb_hi = ca.astype(bf16).astype(f32), cb.astype(bf16).astype(f32)
    wide = iota((B, D), 1)
    mixed = jnp.where((wide == 0) | (wide == 8), ca_hi, jnp.where((wide == 1) | (wide == 9), cb_hi, 0.0))
    mixed = jnp.where(wide == 16, ca - ca_hi, jnp.where(wide == 17, cb - cb_hi, mixed))
    colm[...] = mixed[:, :32].astype(bf16)
    rows[0:1] = influence(lw, float(B), k)
    rows[1:2] = influence(lw, float(B), B - 1.0 - k)
    gwf[...] = wi[0]
    hi, lo = split(wi[0])
    gw3[:, :B] = hi
    gw3[:, B : 2 * B] = hi
    gw3[:, 2 * B :] = lo
    hi, lo = split(di[0].T)
    gd4[:D, :D] = hi
    gd4[:D, D:] = lo
    gd4[D:, :D] = hi
    gd4[D:, D:] = jnp.zeros((D, D), bf16)
    ad, bd = influence(ld, float(D), k), influence(ld, float(D), D - 1.0 - k)
    line = iota((2 * H, D), 0)
    for h in range(H):
        v = jnp.where(line == h, ad, jnp.where(line == H + h, bd, 0.0))
        hi, lo = split(v)
        at = slice(h * D, (h + 1) * D)
        spread[: 2 * H, at] = hi
        spread[2 * H : 4 * H, at] = hi
        spread[4 * H :, at] = lo
    a = iota((2 * H, 128), 0)
    b = iota((2 * H, 128), 1)
    af = lax.bitwise_and(a, H - 1).astype(f32)
    bfl = lax.bitwise_and(b, H - 1).astype(f32)
    wide_h = jnp.broadcast_to(lh, (2 * H, 128))
    g = green(jnp.broadcast_to(sh, (2 * H, 128)), wide_h, float(H), af, bfl)
    hmat[...] = jnp.where((b < 2 * H) & (lax.shift_right_logical(a, 4) == lax.shift_right_logical(b, 4)), g, 0.0)
    c = iota((H, 128), 0).astype(f32)
    ln = iota((H, 128), 1)
    hcol[...] = influence(jnp.broadcast_to(lh, (H, 128)), float(H), jnp.where(ln == 0, c, H - 1.0 - c))


def sums_kernel(cpl_far, rho, sig, cr, cs, halo, rv, sv, coef, packed, cpl, sems, sem):
    small = pltpu.make_async_copy(cpl_far, cpl, sem)
    small.start()
    def parts(i):
        at = pl.ds(pl.multiple_of(i * B, B), B)
        return (
            pltpu.make_async_copy(rho.at[:, at, :], rv.at[:, at, :], sems.at[0, i]),
            pltpu.make_async_copy(sig.at[:, at, :], sv.at[:, at, :], sems.at[1, i]),
        )

    for i in range(NB):
        for part in parts(i):
            part.start()
    small.wait()
    sh = jnp.full((8, 128), cpl[1], f32)
    lh = log_decay(sh)
    for h in range(H):
        coef[h] = influence(lh, float(H), float(h)) / sh

    R = 32
    lane = iota((R, D), 1)

    def block(i, _):
        for part in parts(i):
            part.wait()
        packs, combs = [], []
        for t in range(B // R):
            at = pl.ds(pl.multiple_of(i * B + t * R, R), R)
            fr = jnp.zeros((R, D), f32)
            tr, fs, ts, pack = fr, fr, fr, fr
            for h in range(H):
                x, y = rv[h, at, :], sv[h, at, :]
                cf = jnp.broadcast_to(coef[h, 0:1, :], (R, D))
                ct = jnp.broadcast_to(coef[H - 1 - h, 0:1, :], (R, D))
                fr, tr, fs, ts = fr + cf * x, tr + ct * x, fs + cf * y, ts + ct * y
                pack = jnp.where((lane == 2 * h) | (lane == 2 * h + 1), pltpu.roll(x, 2 * h + 1, 1), pack)
            cr[0, at, :], cr[1, at, :], cs[0, at, :], cs[1, at, :] = fr, tr, fs, ts
            packs.append(pack)
            combs.append(jnp.where(lane < 2, pltpu.roll(fr, 1, 1), pltpu.roll(tr, 3, 1)))
        at = pl.ds(pl.multiple_of(i * B, B), B)
        packed[...] = jnp.concatenate(packs, axis=0).T[: 2 * H]
        halo[:H, at] = packed[pl.ds(1, H, stride=2), :]
        halo[H : 2 * H, at] = packed[pl.ds(0, H, stride=2), :]
        halo[2 * H :, at] = jnp.concatenate(combs, axis=0).T[:8]
        return 0

    lax.fori_loop(0, NB, block, 0)


def chain_w(yf, yt, par):
    p, q = par[HEAD, 3], par[HEAD, 4]
    before, inv, w, qw = (BEFORE_W + k for k in range(4))
    us = []
    for k in range(NB):
        u = yt[k] + par[w, k] * yf[k]
        us.append(u if k == 0 else u + par[qw, k] * us[-1])
    fs = [None] * NB
    for k in reversed(range(NB)):
        g = yf[k]
        if k > 0:
            g = g + p * us[k - 1]
        if k < NB - 1:
            g = g + q * fs[k + 1]
        fs[k] = g * par[inv, k]
    zero = jnp.zeros_like(yf[0])
    ls = [zero] + [us[k - 1] + par[before, k] * fs[k] for k in range(1, NB)]
    return ls, fs[1:] + [zero]


def solve_wd(x, gw3, gd4):
    hi, lo = split(x)
    z = dot(gw3[:, : 2 * B], jnp.concatenate([hi, lo], axis=0)) + dot(gw3[:, 2 * B :], hi)
    z = jnp.concatenate([z[:, :D], z[:, D:]], axis=0)
    hi, lo = split(z)
    y = dot(jnp.concatenate([hi, lo], axis=1), gd4[...])
    return y[:, :D] + y[:, D:]


def edges_kernel(par, cr, cs, from_left, from_right, gw3, gd4, cols, out, e):
    c0, c1, c2 = par[HEAD, 0], par[HEAD, 1], par[HEAD, 2]
    row = iota((B, D), 0)
    lane = iota((B, D), 1)
    blank = jnp.zeros((B - 8, B), f32)
    for k in range(NB):
        spot = slice(k * B, (k + 1) * B)
        lc = jnp.concatenate([from_left[2 * H :, spot], blank], axis=0).T
        rc = jnp.concatenate([from_right[2 * H :, spot], blank], axis=0).T
        xs = []
        for j in range(2):
            x = cr[j, spot]
            up = pltpu.roll(x, 1, 0)
            up = jnp.where(row == 0, cr[j, k * B - 1 : k * B] if k > 0 else 0.0, up)
            down = pltpu.roll(x, B - 1, 0)
            down = jnp.where(row == B - 1, cr[j, (k + 1) * B : (k + 1) * B + 1] if k < NB - 1 else 0.0, down)
            lcol = lc if j == 0 else pltpu.roll(lc, D - 2, 1)
            left = jnp.where(lane == 0, lcol, pltpu.roll(x, 1, 1))
            right = jnp.where(lane == D - 1, pltpu.roll(rc, D - 2 if j == 0 else D - 4, 1), pltpu.roll(x, D - 1, 1))
            xs.append(cs[j, spot] + c0 * x + c1 * (up + down) + c2 * (left + right))
        y = solve_wd(jnp.concatenate(xs, axis=1), gw3, gd4)
        e[0, spot] = y[:B]
        e[1, spot] = y[B:]
    for j in range(2):
        ls, rs = chain_w(
            [e[j, k * B : k * B + 1] for k in range(NB)], [e[j, k * B + B - 1 : k * B + B] for k in range(NB)], par
        )
        for k in range(NB):
            spot = slice(k * B, (k + 1) * B)
            e[j, spot] = e[j, spot] + cols[0] * ls[k] + cols[1] * rs[k]
        for p in range(NP):
            out[p, S * j : S * (j + 1)] = e[j, S * p : S * (p + 1)]


def field_kernel(start, count, par, rho, sig, gw3, gd4, raw, ew, qp, rv, out, packed, sems, rims):
    sv = out

    def place(i, lead=0):
        return pl.ds(pl.multiple_of(i * B + lead, 8), B)

    def parts(i):
        there = place(i, start * B)
        return (
            pltpu.make_async_copy(rho.at[:, there, :], rv.at[:, place(i, 8), :], sems.at[0, i]),
            pltpu.make_async_copy(sig.at[:, there, :], out.at[:, place(i), :], sems.at[1, i]),
        )

    def send(i):
        return pltpu.make_async_copy(out.at[:, place(i), :], raw.at[:, place(i), :], sems.at[2, i])

    ends = []
    if start > 0:
        ends.append((start * B - 8, 0))
    if start + count < NB:
        ends.append(((start + count) * B, 8 + count * B))
    ends = [
        pltpu.make_async_copy(rho.at[:, pl.ds(there, 8), :], rv.at[:, pl.ds(here, 8), :], rims.at[n])
        for n, (there, here) in enumerate(ends)
    ]
    for end in ends:
        end.start()
    for i in range(count):
        for part in parts(i):
            part.start()
    for end in ends:
        end.wait()
    for part in parts(0):
        part.wait()
    c0, c1, c2 = par[HEAD, 0], par[HEAD, 1], par[HEAD, 2]
    row = iota((B, D), 0)
    half = H // 2
    meet = par[HEAD, 9]

    def block(i, _):
        @pl.when(i < count - 1)
        def _():
            for part in parts(jnp.minimum(i + 1, count - 1)):
                part.wait()

        here = place(i)
        inner = place(i, 8)
        before = pl.ds(pl.multiple_of(i * B, 8), 8)
        after = pl.ds(pl.multiple_of(i * B + B + 8, 8), 8)
        for h in range(H):
            x = rv[h, inner, :]
            first = jnp.where(i + start > 0, rv[h, before, :][7:8], 0.0)
            last = jnp.where(i + start < NB - 1, rv[h, after, :][0:1], 0.0)
            up = jnp.where(row == 0, first, pltpu.roll(x, 1, 0))
            down = jnp.where(row == B - 1, last, pltpu.roll(x, B - 1, 0))
            out[h, here, :] = (
                sv[h, here, :] + c0 * x + c1 * (up + down) + c2 * (pltpu.roll(x, 1, 1) + pltpu.roll(x, D - 1, 1))
            )

        def tile(j, _):
            at = pl.ds(pl.multiple_of(i * B + T * j, T), T)
            beside = pl.ds(pl.multiple_of(i * B + T * j + 8, 8), T)
            top, bottom = [None] * half, [None] * half
            for h in range(half):
                m, c = par[MH, h], par[CH, h]
                a, b = m * out[h, at, :], m * out[H - 1 - h, at, :]
                top[h] = a if h == 0 else a + c * top[h - 1]
                bottom[h] = b if h == 0 else b + c * bottom[h - 1]
            c = par[CH, half - 1]
            x = (top[half - 1] + c * bottom[half - 1]) * meet
            y = bottom[half - 1] + c * x
            for h in reversed(range(half)):
                if h < half - 1:
                    c = par[CH, h]
                    x, y = top[h] + c * x, bottom[h] + c * y
                out[h, at, :] = x - 2.0 * rv[h, beside, :]
                out[H - 1 - h, at, :] = y - 2.0 * rv[H - 1 - h, beside, :]
            return 0

        lax.fori_loop(0, B // T, tile, 0)
        lane = iota((B, D), 1)
        pack = jnp.zeros((B, D), f32)
        for g in range(H // 2):
            y = solve_wd(jnp.concatenate([out[2 * g, here, :], out[2 * g + 1, here, :]], axis=1), gw3, gd4)
            for side in range(2):
                h = 2 * g + side
                part = y[side * B : (side + 1) * B]
                ew[i, 0, h : h + 1, :] = part[0:1]
                ew[i, 1, h : h + 1, :] = part[B - 1 : B]
                out[h, here, :] = part + rv[h, inner, :]
                pack = jnp.where((lane == 2 * h) | (lane == 2 * h + 1), pltpu.roll(part, 2 * h + 1, 1), pack)
        packed[...] = pack.T[: 2 * H]
        qp[:H, here] = packed[pl.ds(1, H, stride=2), :]
        qp[H:, here] = packed[pl.ds(0, H, stride=2), :]
        send(i).start()
        return 0

    lax.fori_loop(0, count, block, 0)
    for i in range(count):
        send(i).wait()


def planes_kernel(par, ew0, ew1, qp0, qp1, own, from_left, from_right, hmat, rows, gwf, planes, u, fix, flat):
    ew = [ew0[k] for k in range(HALF)] + [ew1[k] for k in range(NB - HALF)]
    ls, rs = chain_w([a[0] for a in ew], [a[1] for a in ew], par)
    flat[...] = jnp.zeros((8, H * D), f32)
    for k in range(NB):
        for h in range(H):
            flat[0:1, h * D : (h + 1) * D] = ls[k][h : h + 1]
            flat[1:2, h * D : (h + 1) * D] = rs[k][h : h + 1]
        x = flat[...]
        hi = x.astype(bf16).astype(f32)
        fix[k] = jnp.concatenate([hi, x - hi, hi, jnp.zeros_like(x)], axis=0).astype(bf16)
    v = jnp.concatenate([from_left[H : 2 * H] - own[H : 2 * H], from_right[:H] - own[:H]], axis=0)
    v = jnp.dot(hmat[:, : 2 * H], v, precision=HIGHEST, preferred_element_type=f32)
    parts = []
    for k in range(NB):
        spot = slice(k * B, (k + 1) * B)
        solved = lax.dot_general(
            v[:, spot], gwf[...], (((1,), (1,)), ((), ())), precision=HIGHEST, preferred_element_type=f32
        )
        seen = qp0[:, spot] if k < HALF else qp1[:, (k - HALF) * B : (k - HALF + 1) * B]
        parts.append(jnp.concatenate([2.0 * solved, seen], axis=0))
    ls, rs = chain_w([a[:, 0:1] for a in parts], [a[:, B - 1 : B] for a in parts], par)
    p, q = par[HEAD, 7], par[HEAD, 8]
    for k in range(NB):
        spot = slice(k * B, (k + 1) * B)
        both = parts[k] + ls[k] * rows[0:1] + rs[k] * rows[1:2]
        ul, ur = both[:H], both[H : 2 * H]
        u[:, spot] = both[: 2 * H]
        planes[:H, spot] = both[2 * H : 3 * H] + p * ul + q * ur
        planes[H:, spot] = both[3 * H :] + q * ul + p * ur


def pair_kernel(par, a, b, out):
    def joined(first, last):
        return (
            par[PAIR, 0] * a[first, :] + par[PAIR, 1] * a[last, :] + par[PAIR, 2] * b[first, :] + par[PAIR, 3] * b[last, :]
        )

    out[:H] = joined(pl.ds(0, H), pl.ds(H, H))
    out[H:] = jnp.zeros((8, W), f32)
    for plane in range(2):
        at = 2 * H + 2 * plane
        out[H + plane : H + plane + 1] = joined(pl.ds(at + 1, 1), pl.ds(at, 1))


def solver_kernel(par, y, out, us):
    p, q = par[HEAD, 5], par[HEAD, 6]
    before, inv, w, qw = (BEFORE_H + k for k in range(4))
    u = y[0, S:] + par[w, 0] * y[0, :S]
    us[0] = u
    for k in range(1, NP):
        u = y[k, S:] + par[w, k] * y[k, :S] + par[qw, k] * u
        us[k] = u
    zero = jnp.zeros_like(u)
    out[NP - 1, S:] = zero
    f = zero
    for k in reversed(range(NP)):
        g = y[k, :S]
        if k > 0:
            g = g + p * us[k - 1]
        f = (g + q * f) * par[inv, k]
        if k > 0:
            out[k, :S] = us[k - 1] + par[before, k] * f
            out[k - 1, S:] = f
    out[0, :S] = zero


def corner_kernel(a, planes, out, wide):
    out[: 2 * H] = planes[...]
    lane = iota((S, D), 1)
    for p in range(NP):
        wide[S * p : S * (p + 1)] = jnp.where(lane < 2, pltpu.roll(a[p, :S], 1, 1), pltpu.roll(a[p, S:], 3, 1))
    for k in range(NB):
        out[2 * H :, k * B : (k + 1) * B] = wide[k * B : (k + 1) * B].T[:8]


def nearly_kernel(par, raw0, raw1, a, out, lr, sems):
    for i in range(NB):
        raw, k = (raw0, i) if i < HALF else (raw1, i - HALF)
        spot = pl.ds(i * B, B)
        pltpu.make_async_copy(raw.at[:, pl.ds(k * B, B), :], out.at[:, spot, :], sems.at[i]).start()
    for p in range(NP):
        for j in range(2):
            lr[j, S * p : S * (p + 1)] = a[p, S * j : S * (j + 1)]

    def block(i, _):
        at = pl.ds(pl.multiple_of(i * B, B), B)
        pltpu.make_async_copy(raw1.at[:, pl.ds(0, B), :], out.at[:, at, :], sems.at[i]).wait()
        l, r = lr[0, at, :], lr[1, at, :]
        for h in range(H):
            out[h, at, :] = out[h, at, :] + (par[AH, h] * l + par[AH, H - 1 - h] * r)
        return 0

    lax.fori_loop(0, NB, block, 0)


def final_kernel(par, base, fix, colm, a, b, v0, v1, u, hcol, spread, out, tall, buf, sems):
    beyond = par[HEAD, 10] * v1[...] + par[HEAD, 11] * v0[...]

    def known(first, last, far_row):
        return (a[first, :], a[last, :], b[first, :], b[last, :], far_row)

    sides = []
    for side in range(2):

        def mixed(parts):
            total = 0.0
            for k, part in enumerate(parts):
                total = total + par[PAIR + 1 + side, k] * part
            return total

        own = u[H * side : H * (side + 1)] + mixed(known(pl.ds(0, H), pl.ds(H, H), beyond[:H]))
        for plane in range(2):
            at = 2 * H + 2 * plane
            row = beyond[H + plane : H + plane + 1]
            own = own + hcol[:, plane : plane + 1] * mixed(known(pl.ds(at + 1, 1), pl.ds(at, 1), row))
        sides.append(own)
    both = jnp.concatenate(sides + [jnp.zeros((D - 2 * H, W), f32)], axis=0)
    for k in range(NB):
        tall[k * B : (k + 1) * B] = both[:, k * B : (k + 1) * B].T

    def send(i):
        at = pl.ds(pl.multiple_of(i * B, B), B)
        return pltpu.make_async_copy(buf.at[:, at, :], out.at[:, at, :], sems.at[i])

    def block(i, _):
        at = pl.ds(pl.multiple_of(i * B, B), B)
        hi, lo = split(tall[at, : 2 * H])
        wide = dot(
            jnp.concatenate([hi, lo, hi, colm[...]], axis=1), jnp.concatenate([spread[...], fix[i]], axis=0)
        )
        for h in range(H):
            buf[h, at, :] = base[h, at, :] + wide[:, h * D : (h + 1) * D]
        send(i).start()
        return 0

    lax.fori_loop(0, NB, block, 0)
    for i in range(NB):
        send(i).wait()


SMEM = pl.BlockSpec(memory_space=pltpu.SMEM)
VMEM = pl.BlockSpec(memory_space=pltpu.VMEM)
HBM = pl.BlockSpec(memory_space=pltpu.HBM)


def limit(mib):
    return pltpu.CompilerParams(vmem_limit_bytes=mib * 2**20)


def held(*shape, dtype=f32):
    return pltpu.VMEM(shape, dtype)


def near(x):
    return pltpu.with_memory_space_constraint(x, pltpu.VMEM)


def far(x):
    return pltpu.with_memory_space_constraint(x, pltpu.HBM)


def cost(flops, bytes_accessed):
    return pl.CostEstimate(flops=flops, bytes_accessed=bytes_accessed, transcendentals=0)


def per_device(density, source, coupling, width_inverse, height_inverse, depth_inverse):
    slab = lax.axis_index("slab")
    slabs = lax.axis_size("slab")
    up = [(k, k + 1) for k in range(slabs - 1)]
    down = [(k + 1, k) for k in range(slabs - 1)]
    grid = [pltpu.VMEM((H, W + 8, D), f32)]

    cr, cs, halo = pl.pallas_call(
        sums_kernel,
        in_specs=[HBM, HBM, HBM],
        out_specs=[VMEM] * 3,
        out_shape=[held(2, W, D), held(2, W, D), held(2 * H + 8, W)],
        scratch_shapes=grid * 2
        + [
            pltpu.VMEM((H, 8, 128), f32),
            pltpu.VMEM((2 * H, B), f32),
            pltpu.SMEM((3,), f32),
            pltpu.SemaphoreType.DMA((2, NB)),
            pltpu.SemaphoreType.DMA(()),
        ],
        compiler_params=limit(24),
        name="sums",
        cost_estimate=cost(10**7, 14 * 10**6),
    )(far(coupling), far(density), far(source))
    halo_left = lax.ppermute(halo, "slab", up)
    halo_right = lax.ppermute(halo, "slab", down)

    first = pl.BlockSpec((1, B, B), lambda *_: (0, 0, 0))
    shapes = [
        ((16, 128), f32),
        ((2, B, D), f32),
        ((8, 128), f32),
        ((B, 3 * B), bf16),
        ((2 * D, 2 * D), bf16),
        ((6 * H, H * D), bf16),
        ((2 * H, 128), f32),
        ((H, 128), f32),
        ((B, B), f32),
        ((B, 32), bf16),
    ]
    par, cols, rows, gw3, gd4, spread, hmat, hcol, gwf, colm = pl.pallas_call(
        tables_kernel,
        grid=(1,),
        in_specs=[SMEM, SMEM, first, first],
        out_specs=[pl.BlockSpec(shape, lambda *_, n=len(shape): (0,) * n) for shape, _ in shapes],
        out_shape=[jax.ShapeDtypeStruct(*shapes[0])] + [held(*shape, dtype=kind) for shape, kind in shapes[1:]],
        compiler_params=limit(8),
        name="tables",
        cost_estimate=cost(10**7, 10**6),
    )(coupling, slab.reshape(1), width_inverse, depth_inverse)

    edges = pl.pallas_call(
        edges_kernel,
        in_specs=[SMEM] + [VMEM] * 7,
        out_specs=VMEM,
        out_shape=held(NP, 2 * S, D),
        scratch_shapes=[pltpu.VMEM((2, W, D), f32)],
        compiler_params=limit(8),
        name="edges",
        cost_estimate=cost(10**8, 3 * 10**6),
    )(par, near(cr), near(cs), near(halo_left), near(halo_right), near(gw3), near(gd4), near(cols))
    arrived = lax.all_to_all(edges, "pencil", 0, 0, tiled=True)

    def field(start, count):
        rows = count * B
        return pl.pallas_call(
            partial(field_kernel, start, count),
            in_specs=[SMEM, HBM, HBM, VMEM, VMEM],
            out_specs=[HBM, VMEM, VMEM],
            out_shape=[pltpu.HBM((H, rows, D), f32), held(count, 2, H, D), held(2 * H, rows)],
            scratch_shapes=[
                pltpu.VMEM((H, rows + 16, D), f32),
                pltpu.VMEM((H, rows, D), f32),
                pltpu.VMEM((2 * H, B), f32),
                pltpu.SemaphoreType.DMA((3, count)),
                pltpu.SemaphoreType.DMA((2,)),
            ],
            compiler_params=limit(24),
            name="field" + str(start),
            cost_estimate=cost(2 * 10**9, 10**7),
        )(par, far(density), far(source), near(gw3), near(gd4))

    raw0, ew0, qp0 = field(0, HALF)
    arrived, ew0 = lax.optimization_barrier((arrived, ew0))
    solved = pl.pallas_call(
        solver_kernel,
        in_specs=[SMEM, VMEM],
        out_specs=VMEM,
        out_shape=held(NP, 2 * S, D),
        scratch_shapes=[pltpu.VMEM((NP, S, D), f32)],
        compiler_params=limit(8),
        name="solver",
        cost_estimate=cost(10**6, 2 * 10**6),
    )(par, near(arrived))
    outside = lax.all_to_all(solved, "pencil", 0, 0, tiled=True)

    raw1, ew1, qp1 = field(HALF, NB - HALF)
    planes, u, fix = pl.pallas_call(
        planes_kernel,
        in_specs=[SMEM] + [VMEM] * 10,
        out_specs=[VMEM] * 3,
        out_shape=[held(2 * H, W), held(2 * H, W), held(NB, 32, H * D, dtype=bf16)],
        scratch_shapes=[pltpu.VMEM((8, H * D), f32)],
        compiler_params=limit(8),
        name="planes",
        cost_estimate=cost(10**8, 10**6),
    )(par, *[near(v) for v in (ew0, ew1, qp0, qp1)], near(halo), near(halo_left), near(halo_right), near(hmat), near(rows), near(gwf))

    outside = near(outside)
    corners = pl.pallas_call(
        corner_kernel,
        in_specs=[VMEM] * 2,
        out_specs=VMEM,
        out_shape=held(2 * H + 8, W),
        scratch_shapes=[pltpu.VMEM((W, D), f32)],
        compiler_params=limit(8),
        name="corner",
        cost_estimate=cost(10**6, 10**6),
    )(outside, near(planes))

    def across(value, d):
        return lax.ppermute(value, "slab", [(k, k ^ d) for k in range(slabs)])

    beside = across(corners, 1)
    rim = pl.pallas_call(
        pair_kernel,
        in_specs=[SMEM] + [VMEM] * 2,
        out_specs=VMEM,
        out_shape=held(H + 8, W),
        compiler_params=limit(8),
        name="pair",
        cost_estimate=cost(10**5, 10**5),
    )(par, near(corners), near(beside))
    far_rim = across(rim, 2)
    base = pl.pallas_call(
        nearly_kernel,
        in_specs=[SMEM, HBM, HBM, VMEM],
        out_specs=VMEM,
        out_shape=held(H, W, D),
        scratch_shapes=[pltpu.VMEM((2, W, D), f32), pltpu.SemaphoreType.DMA((NB,))],
        compiler_params=limit(8),
        name="nearly",
        cost_estimate=cost(10**8, 7 * 10**6),
    )(par, far(raw0), far(raw1), outside)
    return pl.pallas_call(
        final_kernel,
        in_specs=[SMEM] + [VMEM] * 10,
        out_specs=HBM,
        out_shape=pltpu.HBM((H, W, D), f32),
        scratch_shapes=[pltpu.VMEM((W, D), f32), *grid, pltpu.SemaphoreType.DMA((NB,))],
        compiler_params=limit(16),
        name="final",
        cost_estimate=cost(10**9, 13 * 10**6),
    )(
        par,
        near(base),
        near(fix),
        near(colm),
        near(corners),
        near(beside),
        near(rim),
        near(far_rim),
        near(u),
        near(hcol),
        near(spread),
    )


def solution(mesh):
    in_specs = (P("pencil", None, "slab"), P("pencil", None, "slab"), P(), P(), P(), P())
    out_specs = P("pencil", None, "slab")
    return jax.shard_map(per_device, mesh=mesh, in_specs=in_specs, out_specs=out_specs, check_vma=False)
```

```python
from functools import partial

import jax
import jax.numpy as jnp
from jax import lax
from jax.experimental import pallas as pl
from jax.experimental.pallas import tpu as pltpu
from jax.sharding import PartitionSpec as P

H, W, D = 16, 768, 128
B = 128
NB = W // B
NP = 32
S = W // NP
T = 32
HALF = 3
f32 = jnp.float32
bf16 = jnp.bfloat16
HIGHEST = lax.Precision.HIGHEST


def log_decay(s):
    return jnp.log(2.0 * s / (1.0 + 2.0 * s + jnp.sqrt(1.0 + 4.0 * s)))


def pivots(log_r, length):
    return (
        jnp.exp(log_r)
        * (1.0 - jnp.exp(log_r * (2.0 * length)))
        / (1.0 - jnp.exp(log_r * (2.0 * length + 2.0)))
    )


def influence(log_r, m, i):
    return (
        jnp.exp(log_r * (i + 1.0))
        * (1.0 - jnp.exp(log_r * (2.0 * (m - i))))
        / (1.0 - jnp.exp(log_r * (2.0 * m + 2.0)))
    )


def green(s, log_r, n, i, j):
    low, high = jnp.minimum(i, j), jnp.maximum(i, j)
    return (
        jnp.exp(log_r * (high - low))
        * (1.0 - jnp.exp(log_r * (2.0 * low + 2.0)))
        * (1.0 - jnp.exp(log_r * (2.0 * (n - high))))
        / (jnp.sqrt(1.0 + 4.0 * s) * (1.0 - jnp.exp(log_r * (2.0 * n + 2.0))))
    )


def split(x):
    hi = x.astype(bf16)
    return hi, (x - hi.astype(f32)).astype(bf16)


def dot(a, b):
    return lax.dot_general(a, b, (((1,), (0,)), ((), ())), preferred_element_type=f32)


def iota(shape, dim):
    return lax.broadcasted_iota(jnp.int32, shape, dim)


HEAD, BEFORE_H, BEFORE_W, AH, CH, MH, PAIR = 0, 1, 5, 9, 10, 11, 12


def tables_kernel(cpl, slab, wi, di, par, cols, rows, gw3, gd4, spread, hmat, hcol, gwf, colm):
    row = (1, 128)
    sw, sh, sd = (jnp.full(row, cpl[k], f32) for k in range(3))
    lw, lh, ld = log_decay(sw), log_decay(sh), log_decay(sd)
    lane = iota(row, 1)
    k = lane.astype(f32)
    heads = [2.0 - 4.0 * sw - 4.0 * sd, 2.0 * sw, 2.0 * sd]
    for log_r, m in ((lw, float(B)), (lh, float(H)), (ld, float(D))):
        heads += [influence(log_r, m, 0.0), influence(log_r, m, m - 1.0)]
    middle = pivots(lh, float(H // 2))
    heads.append(1.0 / (1.0 - middle * middle))
    p, q = heads[7], heads[8]
    i1 = 1.0 / (1.0 - p * p)
    v = p + p * q * q * i1
    i2 = 1.0 / (1.0 - v * v)
    heads += [i2, i2 * v, jnp.full(row, lax.bitwise_and(slab[0], 1), jnp.int32).astype(f32)]
    one, none = jnp.ones(row, f32), jnp.zeros(row, f32)
    by_slab = (
        ((none, q * i1, q * i1 * p, one, none), (none,) * 5, (none, p * i1, i1, none, q * i1)),
        ((q * i1 * p, one, none, q * i1, none), (p * i1, none, none, i1, p * q * i1), (none,) * 4 + (one,)),
        ((one, q * i1 * p, q * i1, none, none), (none,) * 4 + (one,), (none, p * i1, i1, none, p * q * i1)),
        ((q * i1, none, one, q * i1 * p, none), (p * i1, none, none, i1, q * i1), (none,) * 5),
    )
    mine = jnp.full(row, slab[0], jnp.int32)
    for line in range(3):
        total = none
        for at in range(4):
            for n, value in enumerate(by_slab[at][line]):
                total = jnp.where((mine == at) & (lane == n), value, total)
        par[PAIR + line : PAIR + line + 1] = total
    head = jnp.zeros(row, f32)
    for at, v in enumerate(heads):
        head = jnp.where(lane == at, v, head)
    par[HEAD : HEAD + 1] = head
    for at, log_r, m, p, q in ((BEFORE_H, lh, float(H), heads[5], heads[6]), (BEFORE_W, lw, float(B), heads[3], heads[4])):
        before = pivots(log_r, m * k)
        inv = 1.0 / (1.0 - p * before)
        w = q * before * inv
        for n, v in enumerate((before, inv, w, q + w * p)):
            par[at + n : at + n + 1] = v
    kc = jnp.minimum(k, H - 1.0)
    ch = pivots(lh, kc + 1.0)
    par[AH : AH + 1] = influence(lh, float(H), kc)
    par[CH : CH + 1] = ch
    par[MH : MH + 1] = ch / sh
    tall = iota((B, D), 0).astype(f32)
    lww = jnp.broadcast_to(lw, (B, D))
    cols[0] = influence(lww, float(B), tall)
    cols[1] = influence(lww, float(B), B - 1.0 - tall)
    ca, cb = cols[0], cols[1]
    ca_hi, cb_hi = ca.astype(bf16).astype(f32), cb.astype(bf16).astype(f32)
    wide = iota((B, D), 1)
    mixed = jnp.where((wide == 0) | (wide == 8), ca_hi, jnp.where((wide == 1) | (wide == 9), cb_hi, 0.0))
    mixed = jnp.where(wide == 16, ca - ca_hi, jnp.where(wide == 17, cb - cb_hi, mixed))
    colm[...] = mixed[:, :32].astype(bf16)
    rows[0:1] = influence(lw, float(B), k)
    rows[1:2] = influence(lw, float(B), B - 1.0 - k)
    gwf[...] = wi[0]
    hi, lo = split(wi[0])
    gw3[:, :B] = hi
    gw3[:, B : 2 * B] = hi
    gw3[:, 2 * B :] = lo
    hi, lo = split(di[0].T)
    gd4[:D, :D] = hi
    gd4[:D, D:] = lo
    gd4[D:, :D] = hi
    gd4[D:, D:] = jnp.zeros((D, D), bf16)
    ad, bd = influence(ld, float(D), k), influence(ld, float(D), D - 1.0 - k)
    line = iota((2 * H, D), 0)
    for h in range(H):
        v = jnp.where(line == h, ad, jnp.where(line == H + h, bd, 0.0))
        hi, lo = split(v)
        at = slice(h * D, (h + 1) * D)
        spread[: 2 * H, at] = hi
        spread[2 * H : 4 * H, at] = hi
        spread[4 * H :, at] = lo
    a = iota((2 * H, 128), 0)
    b = iota((2 * H, 128), 1)
    af = lax.bitwise_and(a, H - 1).astype(f32)
    bfl = lax.bitwise_and(b, H - 1).astype(f32)
    wide_h = jnp.broadcast_to(lh, (2 * H, 128))
    g = green(jnp.broadcast_to(sh, (2 * H, 128)), wide_h, float(H), af, bfl)
    hmat[...] = jnp.where((b < 2 * H) & (lax.shift_right_logical(a, 4) == lax.shift_right_logical(b, 4)), g, 0.0)
    c = iota((H, 128), 0).astype(f32)
    ln = iota((H, 128), 1)
    hcol[...] = influence(jnp.broadcast_to(lh, (H, 128)), float(H), jnp.where(ln == 0, c, H - 1.0 - c))


def sums_kernel(cpl_far, slab_far, rho, sig, cr, cs, inner, outer, rv, sv, coef, packed, cpl, slab, sems, sem):
    small = pltpu.make_async_copy(cpl_far, cpl, sem.at[0])
    small.start()
    where = pltpu.make_async_copy(slab_far, slab, sem.at[1])
    where.start()
    def parts(i):
        at = pl.ds(pl.multiple_of(i * B, B), B)
        return (
            pltpu.make_async_copy(rho.at[:, at, :], rv.at[:, at, :], sems.at[0, i]),
            pltpu.make_async_copy(sig.at[:, at, :], sv.at[:, at, :], sems.at[1, i]),
        )

    for i in range(NB):
        for part in parts(i):
            part.start()
    small.wait()
    where.wait()
    odd = lax.bitwise_and(slab[0], 1) == 1
    sh = jnp.full((8, 128), cpl[1], f32)
    lh = log_decay(sh)
    for h in range(H):
        coef[h] = influence(lh, float(H), float(h)) / sh

    R = 32
    lane = iota((R, D), 1)

    def block(i, _):
        for part in parts(i):
            part.wait()
        packs, combs = [], []
        for t in range(B // R):
            at = pl.ds(pl.multiple_of(i * B + t * R, R), R)
            fr = jnp.zeros((R, D), f32)
            tr, fs, ts, pack = fr, fr, fr, fr
            for h in range(H):
                x, y = rv[h, at, :], sv[h, at, :]
                cf = jnp.broadcast_to(coef[h, 0:1, :], (R, D))
                ct = jnp.broadcast_to(coef[H - 1 - h, 0:1, :], (R, D))
                fr, tr, fs, ts = fr + cf * x, tr + ct * x, fs + cf * y, ts + ct * y
                pack = jnp.where((lane == 2 * h) | (lane == 2 * h + 1), pltpu.roll(x, 2 * h + 1, 1), pack)
            cr[0, at, :], cr[1, at, :], cs[0, at, :], cs[1, at, :] = fr, tr, fs, ts
            packs.append(pack)
            combs.append(jnp.where(lane < 2, pltpu.roll(fr, 1, 1), pltpu.roll(tr, 3, 1)))
        at = pl.ds(pl.multiple_of(i * B, B), B)
        packed[...] = jnp.concatenate(packs, axis=0).T[: 2 * H]
        first, last = packed[pl.ds(1, H, stride=2), :], packed[pl.ds(0, H, stride=2), :]
        inner[:H, at] = jnp.where(odd, first, last)
        outer[:H, at] = jnp.where(odd, last, first)
        comb = jnp.concatenate(combs, axis=0).T[:8]
        inner[H:, at] = comb
        outer[H:, at] = comb
        return 0

    lax.fori_loop(0, NB, block, 0)


def chain_w(yf, yt, par):
    p, q = par[HEAD, 3], par[HEAD, 4]
    before, inv, w, qw = (BEFORE_W + k for k in range(4))
    us = []
    for k in range(NB):
        u = yt[k] + par[w, k] * yf[k]
        us.append(u if k == 0 else u + par[qw, k] * us[-1])
    fs = [None] * NB
    for k in reversed(range(NB)):
        g = yf[k]
        if k > 0:
            g = g + p * us[k - 1]
        if k < NB - 1:
            g = g + q * fs[k + 1]
        fs[k] = g * par[inv, k]
    zero = jnp.zeros_like(yf[0])
    ls = [zero] + [us[k - 1] + par[before, k] * fs[k] for k in range(1, NB)]
    return ls, fs[1:] + [zero]


def solve_wd(x, gw3, gd4):
    hi, lo = split(x)
    z = dot(gw3[:, : 2 * B], jnp.concatenate([hi, lo], axis=0)) + dot(gw3[:, 2 * B :], hi)
    z = jnp.concatenate([z[:, :D], z[:, D:]], axis=0)
    hi, lo = split(z)
    y = dot(jnp.concatenate([hi, lo], axis=1), gd4[...])
    return y[:, :D] + y[:, D:]


def edges_kernel(par, cr, cs, from_inner, from_outer, gw3, gd4, cols, out, e):
    c0, c1, c2 = par[HEAD, 0], par[HEAD, 1], par[HEAD, 2]
    row = iota((B, D), 0)
    lane = iota((B, D), 1)
    blank = jnp.zeros((B - 8, B), f32)
    odd = par[HEAD, 12] > 0.5
    for k in range(NB):
        spot = slice(k * B, (k + 1) * B)
        a, b = from_inner[H:, spot], from_outer[H:, spot]
        lc = jnp.concatenate([jnp.where(odd, a, b), blank], axis=0).T
        rc = jnp.concatenate([jnp.where(odd, b, a), blank], axis=0).T
        xs = []
        for j in range(2):
            x = cr[j, spot]
            up = pltpu.roll(x, 1, 0)
            up = jnp.where(row == 0, cr[j, k * B - 1 : k * B] if k > 0 else 0.0, up)
            down = pltpu.roll(x, B - 1, 0)
            down = jnp.where(row == B - 1, cr[j, (k + 1) * B : (k + 1) * B + 1] if k < NB - 1 else 0.0, down)
            lcol = lc if j == 0 else pltpu.roll(lc, D - 2, 1)
            left = jnp.where(lane == 0, lcol, pltpu.roll(x, 1, 1))
            right = jnp.where(lane == D - 1, pltpu.roll(rc, D - 2 if j == 0 else D - 4, 1), pltpu.roll(x, D - 1, 1))
            xs.append(cs[j, spot] + c0 * x + c1 * (up + down) + c2 * (left + right))
        y = solve_wd(jnp.concatenate(xs, axis=1), gw3, gd4)
        e[0, spot] = y[:B]
        e[1, spot] = y[B:]
    for j in range(2):
        ls, rs = chain_w(
            [e[j, k * B : k * B + 1] for k in range(NB)], [e[j, k * B + B - 1 : k * B + B] for k in range(NB)], par
        )
        for k in range(NB):
            spot = slice(k * B, (k + 1) * B)
            e[j, spot] = e[j, spot] + cols[0] * ls[k] + cols[1] * rs[k]
        for p in range(NP):
            out[p, S * j : S * (j + 1)] = e[j, S * p : S * (p + 1)]


def field_kernel(start, count, par, rho, sig, gw3, gd4, raw, ew, qp, rv, out, packed, sems, rims):
    sv = out

    def place(i, lead=0):
        return pl.ds(pl.multiple_of(i * B + lead, 8), B)

    def parts(i):
        there = place(i, start * B)
        return (
            pltpu.make_async_copy(rho.at[:, there, :], rv.at[:, place(i, 8), :], sems.at[0, i]),
            pltpu.make_async_copy(sig.at[:, there, :], out.at[:, place(i), :], sems.at[1, i]),
        )

    def send(i):
        return pltpu.make_async_copy(out.at[:, place(i), :], raw.at[:, place(i), :], sems.at[2, i])

    ends = []
    if start > 0:
        ends.append((start * B - 8, 0))
    if start + count < NB:
        ends.append(((start + count) * B, 8 + count * B))
    ends = [
        pltpu.make_async_copy(rho.at[:, pl.ds(there, 8), :], rv.at[:, pl.ds(here, 8), :], rims.at[n])
        for n, (there, here) in enumerate(ends)
    ]
    for end in ends:
        end.start()
    for i in range(count):
        for part in parts(i):
            part.start()
    for end in ends:
        end.wait()
    for part in parts(0):
        part.wait()
    c0, c1, c2 = par[HEAD, 0], par[HEAD, 1], par[HEAD, 2]
    row = iota((B, D), 0)
    half = H // 2
    meet = par[HEAD, 9]

    def block(i, _):
        @pl.when(i < count - 1)
        def _():
            for part in parts(jnp.minimum(i + 1, count - 1)):
                part.wait()

        here = place(i)
        inner = place(i, 8)
        before = pl.ds(pl.multiple_of(i * B, 8), 8)
        after = pl.ds(pl.multiple_of(i * B + B + 8, 8), 8)
        for h in range(H):
            x = rv[h, inner, :]
            first = jnp.where(i + start > 0, rv[h, before, :][7:8], 0.0)
            last = jnp.where(i + start < NB - 1, rv[h, after, :][0:1], 0.0)
            up = jnp.where(row == 0, first, pltpu.roll(x, 1, 0))
            down = jnp.where(row == B - 1, last, pltpu.roll(x, B - 1, 0))
            out[h, here, :] = (
                sv[h, here, :] + c0 * x + c1 * (up + down) + c2 * (pltpu.roll(x, 1, 1) + pltpu.roll(x, D - 1, 1))
            )

        def tile(j, _):
            at = pl.ds(pl.multiple_of(i * B + T * j, T), T)
            beside = pl.ds(pl.multiple_of(i * B + T * j + 8, 8), T)
            top, bottom = [None] * half, [None] * half
            for h in range(half):
                m, c = par[MH, h], par[CH, h]
                a, b = m * out[h, at, :], m * out[H - 1 - h, at, :]
                top[h] = a if h == 0 else a + c * top[h - 1]
                bottom[h] = b if h == 0 else b + c * bottom[h - 1]
            c = par[CH, half - 1]
            x = (top[half - 1] + c * bottom[half - 1]) * meet
            y = bottom[half - 1] + c * x
            for h in reversed(range(half)):
                if h < half - 1:
                    c = par[CH, h]
                    x, y = top[h] + c * x, bottom[h] + c * y
                out[h, at, :] = x - 2.0 * rv[h, beside, :]
                out[H - 1 - h, at, :] = y - 2.0 * rv[H - 1 - h, beside, :]
            return 0

        lax.fori_loop(0, B // T, tile, 0)
        lane = iota((B, D), 1)
        pack = jnp.zeros((B, D), f32)
        for g in range(H // 2):
            y = solve_wd(jnp.concatenate([out[2 * g, here, :], out[2 * g + 1, here, :]], axis=1), gw3, gd4)
            for side in range(2):
                h = 2 * g + side
                part = y[side * B : (side + 1) * B]
                ew[i, 0, h : h + 1, :] = part[0:1]
                ew[i, 1, h : h + 1, :] = part[B - 1 : B]
                out[h, here, :] = part + rv[h, inner, :]
                pack = jnp.where((lane == 2 * h) | (lane == 2 * h + 1), pltpu.roll(part, 2 * h + 1, 1), pack)
        packed[...] = pack.T[: 2 * H]
        qp[:H, here] = packed[pl.ds(1, H, stride=2), :]
        qp[H:, here] = packed[pl.ds(0, H, stride=2), :]
        send(i).start()
        return 0

    lax.fori_loop(0, count, block, 0)
    for i in range(count):
        send(i).wait()


def planes_kernel(par, ew0, ew1, qp0, qp1, inner, outer, from_inner, from_outer, hmat, rows, gwf, planes, u, fix, flat):
    ew = [ew0[k] for k in range(HALF)] + [ew1[k] for k in range(NB - HALF)]
    ls, rs = chain_w([a[0] for a in ew], [a[1] for a in ew], par)
    flat[...] = jnp.zeros((8, H * D), f32)
    for k in range(NB):
        for h in range(H):
            flat[0:1, h * D : (h + 1) * D] = ls[k][h : h + 1]
            flat[1:2, h * D : (h + 1) * D] = rs[k][h : h + 1]
        x = flat[...]
        hi = x.astype(bf16).astype(f32)
        fix[k] = jnp.concatenate([hi, x - hi, hi, jnp.zeros_like(x)], axis=0).astype(bf16)
    odd = par[HEAD, 12] > 0.5
    a, b = from_inner[:H] - outer[:H], from_outer[:H] - inner[:H]
    v = jnp.concatenate([jnp.where(odd, a, b), jnp.where(odd, b, a)], axis=0)
    v = jnp.dot(hmat[:, : 2 * H], v, precision=HIGHEST, preferred_element_type=f32)
    parts = []
    for k in range(NB):
        spot = slice(k * B, (k + 1) * B)
        solved = lax.dot_general(
            v[:, spot], gwf[...], (((1,), (1,)), ((), ())), precision=HIGHEST, preferred_element_type=f32
        )
        seen = qp0[:, spot] if k < HALF else qp1[:, (k - HALF) * B : (k - HALF + 1) * B]
        parts.append(jnp.concatenate([2.0 * solved, seen], axis=0))
    ls, rs = chain_w([a[:, 0:1] for a in parts], [a[:, B - 1 : B] for a in parts], par)
    p, q = par[HEAD, 7], par[HEAD, 8]
    for k in range(NB):
        spot = slice(k * B, (k + 1) * B)
        both = parts[k] + ls[k] * rows[0:1] + rs[k] * rows[1:2]
        ul, ur = both[:H], both[H : 2 * H]
        u[:, spot] = both[: 2 * H]
        planes[:H, spot] = both[2 * H : 3 * H] + p * ul + q * ur
        planes[H:, spot] = both[3 * H :] + q * ul + p * ur


def pair_kernel(par, a, b, out):
    def joined(first, last):
        return (
            par[PAIR, 0] * a[first, :] + par[PAIR, 1] * a[last, :] + par[PAIR, 2] * b[first, :] + par[PAIR, 3] * b[last, :]
        )

    out[:H] = joined(pl.ds(0, H), pl.ds(H, H))
    out[H:] = jnp.zeros((8, W), f32)
    for plane in range(2):
        at = 2 * H + 2 * plane
        out[H + plane : H + plane + 1] = joined(pl.ds(at + 1, 1), pl.ds(at, 1))


def solver_kernel(par, y, out, us):
    p, q = par[HEAD, 5], par[HEAD, 6]
    before, inv, w, qw = (BEFORE_H + k for k in range(4))
    u = y[0, S:] + par[w, 0] * y[0, :S]
    us[0] = u
    for k in range(1, NP):
        u = y[k, S:] + par[w, k] * y[k, :S] + par[qw, k] * u
        us[k] = u
    zero = jnp.zeros_like(u)
    out[NP - 1, S:] = zero
    f = zero
    for k in reversed(range(NP)):
        g = y[k, :S]
        if k > 0:
            g = g + p * us[k - 1]
        f = (g + q * f) * par[inv, k]
        if k > 0:
            out[k, :S] = us[k - 1] + par[before, k] * f
            out[k - 1, S:] = f
    out[0, :S] = zero


def corner_kernel(a, planes, out, wide):
    out[: 2 * H] = planes[...]
    lane = iota((S, D), 1)
    for p in range(NP):
        wide[S * p : S * (p + 1)] = jnp.where(lane < 2, pltpu.roll(a[p, :S], 1, 1), pltpu.roll(a[p, S:], 3, 1))
    for k in range(NB):
        out[2 * H :, k * B : (k + 1) * B] = wide[k * B : (k + 1) * B].T[:8]


def nearly_kernel(par, raw0, raw1, a, out, lr, sems):
    for i in range(NB):
        raw, k = (raw0, i) if i < HALF else (raw1, i - HALF)
        spot = pl.ds(i * B, B)
        pltpu.make_async_copy(raw.at[:, pl.ds(k * B, B), :], out.at[:, spot, :], sems.at[i]).start()
    for p in range(NP):
        for j in range(2):
            lr[j, S * p : S * (p + 1)] = a[p, S * j : S * (j + 1)]

    def block(i, _):
        at = pl.ds(pl.multiple_of(i * B, B), B)
        pltpu.make_async_copy(raw1.at[:, pl.ds(0, B), :], out.at[:, at, :], sems.at[i]).wait()
        l, r = lr[0, at, :], lr[1, at, :]
        for h in range(H):
            out[h, at, :] = out[h, at, :] + (par[AH, h] * l + par[AH, H - 1 - h] * r)
        return 0

    lax.fori_loop(0, NB, block, 0)


def final_kernel(par, base, fix, colm, a, b, v0, v1, u, hcol, spread, out, tall, buf, sems):
    beyond = par[HEAD, 10] * v1[...] + par[HEAD, 11] * v0[...]

    def known(first, last, far_row):
        return (a[first, :], a[last, :], b[first, :], b[last, :], far_row)

    sides = []
    for side in range(2):

        def mixed(parts):
            total = 0.0
            for k, part in enumerate(parts):
                total = total + par[PAIR + 1 + side, k] * part
            return total

        own = u[H * side : H * (side + 1)] + mixed(known(pl.ds(0, H), pl.ds(H, H), beyond[:H]))
        for plane in range(2):
            at = 2 * H + 2 * plane
            row = beyond[H + plane : H + plane + 1]
            own = own + hcol[:, plane : plane + 1] * mixed(known(pl.ds(at + 1, 1), pl.ds(at, 1), row))
        sides.append(own)
    both = jnp.concatenate(sides + [jnp.zeros((D - 2 * H, W), f32)], axis=0)
    for k in range(NB):
        tall[k * B : (k + 1) * B] = both[:, k * B : (k + 1) * B].T

    def send(i):
        at = pl.ds(pl.multiple_of(i * B, B), B)
        return pltpu.make_async_copy(buf.at[:, at, :], out.at[:, at, :], sems.at[i])

    def block(i, _):
        at = pl.ds(pl.multiple_of(i * B, B), B)
        hi, lo = split(tall[at, : 2 * H])
        wide = dot(
            jnp.concatenate([hi, lo, hi, colm[...]], axis=1), jnp.concatenate([spread[...], fix[i]], axis=0)
        )
        for h in range(H):
            buf[h, at, :] = base[h, at, :] + wide[:, h * D : (h + 1) * D]
        send(i).start()
        return 0

    lax.fori_loop(0, NB, block, 0)
    for i in range(NB):
        send(i).wait()


SMEM = pl.BlockSpec(memory_space=pltpu.SMEM)
VMEM = pl.BlockSpec(memory_space=pltpu.VMEM)
HBM = pl.BlockSpec(memory_space=pltpu.HBM)


def limit(mib):
    return pltpu.CompilerParams(vmem_limit_bytes=mib * 2**20)


def held(*shape, dtype=f32):
    return pltpu.VMEM(shape, dtype)


def near(x):
    return pltpu.with_memory_space_constraint(x, pltpu.VMEM)


def far(x):
    return pltpu.with_memory_space_constraint(x, pltpu.HBM)


def cost(flops, bytes_accessed):
    return pl.CostEstimate(flops=flops, bytes_accessed=bytes_accessed, transcendentals=0)


def per_device(density, source, coupling, width_inverse, height_inverse, depth_inverse):
    slab = lax.axis_index("slab")
    slabs = lax.axis_size("slab")

    def across(value, pairs):
        return lax.ppermute(value, "slab", pairs)

    grid = [pltpu.VMEM((H, W + 8, D), f32)]

    cr, cs, inner, outer = pl.pallas_call(
        sums_kernel,
        in_specs=[HBM] * 4,
        out_specs=[VMEM] * 4,
        out_shape=[held(2, W, D), held(2, W, D), held(H + 8, W), held(H + 8, W)],
        scratch_shapes=grid * 2
        + [
            pltpu.VMEM((H, 8, 128), f32),
            pltpu.VMEM((2 * H, B), f32),
            pltpu.SMEM((3,), f32),
            pltpu.SMEM((1,), jnp.int32),
            pltpu.SemaphoreType.DMA((2, NB)),
            pltpu.SemaphoreType.DMA((2,)),
        ],
        compiler_params=limit(24),
        name="sums",
        cost_estimate=cost(10**7, 14 * 10**6),
    )(far(coupling), far(slab.reshape(1)), far(density), far(source))
    from_inner = across(inner, [(k, k ^ 1) for k in range(slabs)])
    from_outer = across(outer, [(1, 2), (2, 1)])

    first = pl.BlockSpec((1, B, B), lambda *_: (0, 0, 0))
    shapes = [
        ((16, 128), f32),
        ((2, B, D), f32),
        ((8, 128), f32),
        ((B, 3 * B), bf16),
        ((2 * D, 2 * D), bf16),
        ((6 * H, H * D), bf16),
        ((2 * H, 128), f32),
        ((H, 128), f32),
        ((B, B), f32),
        ((B, 32), bf16),
    ]
    par, cols, rows, gw3, gd4, spread, hmat, hcol, gwf, colm = pl.pallas_call(
        tables_kernel,
        grid=(1,),
        in_specs=[SMEM, SMEM, first, first],
        out_specs=[pl.BlockSpec(shape, lambda *_, n=len(shape): (0,) * n) for shape, _ in shapes],
        out_shape=[jax.ShapeDtypeStruct(*shapes[0])] + [held(*shape, dtype=kind) for shape, kind in shapes[1:]],
        compiler_params=limit(8),
        name="tables",
        cost_estimate=cost(10**7, 10**6),
    )(coupling, slab.reshape(1), width_inverse, depth_inverse)

    edges = pl.pallas_call(
        edges_kernel,
        in_specs=[SMEM] + [VMEM] * 7,
        out_specs=VMEM,
        out_shape=held(NP, 2 * S, D),
        scratch_shapes=[pltpu.VMEM((2, W, D), f32)],
        compiler_params=limit(8),
        name="edges",
        cost_estimate=cost(10**8, 3 * 10**6),
    )(par, near(cr), near(cs), near(from_inner), near(from_outer), near(gw3), near(gd4), near(cols))
    arrived = lax.all_to_all(edges, "pencil", 0, 0, tiled=True)

    def field(start, count):
        rows = count * B
        return pl.pallas_call(
            partial(field_kernel, start, count),
            in_specs=[SMEM, HBM, HBM, VMEM, VMEM],
            out_specs=[HBM, VMEM, VMEM],
            out_shape=[pltpu.HBM((H, rows, D), f32), held(count, 2, H, D), held(2 * H, rows)],
            scratch_shapes=[
                pltpu.VMEM((H, rows + 16, D), f32),
                pltpu.VMEM((H, rows, D), f32),
                pltpu.VMEM((2 * H, B), f32),
                pltpu.SemaphoreType.DMA((3, count)),
                pltpu.SemaphoreType.DMA((2,)),
            ],
            compiler_params=limit(24),
            name="field" + str(start),
            cost_estimate=cost(2 * 10**9, 10**7),
        )(par, far(density), far(source), near(gw3), near(gd4))

    raw0, ew0, qp0 = field(0, HALF)
    arrived, ew0 = lax.optimization_barrier((arrived, ew0))
    solved = pl.pallas_call(
        solver_kernel,
        in_specs=[SMEM, VMEM],
        out_specs=VMEM,
        out_shape=held(NP, 2 * S, D),
        scratch_shapes=[pltpu.VMEM((NP, S, D), f32)],
        compiler_params=limit(8),
        name="solver",
        cost_estimate=cost(10**6, 2 * 10**6),
    )(par, near(arrived))
    outside = lax.all_to_all(solved, "pencil", 0, 0, tiled=True)

    raw1, ew1, qp1 = field(HALF, NB - HALF)
    planes, u, fix = pl.pallas_call(
        planes_kernel,
        in_specs=[SMEM] + [VMEM] * 11,
        out_specs=[VMEM] * 3,
        out_shape=[held(2 * H, W), held(2 * H, W), held(NB, 32, H * D, dtype=bf16)],
        scratch_shapes=[pltpu.VMEM((8, H * D), f32)],
        compiler_params=limit(8),
        name="planes",
        cost_estimate=cost(10**8, 10**6),
    )(par, *[near(v) for v in (ew0, ew1, qp0, qp1)], near(inner), near(outer), near(from_inner), near(from_outer), near(hmat), near(rows), near(gwf))

    outside = near(outside)
    corners = pl.pallas_call(
        corner_kernel,
        in_specs=[VMEM] * 2,
        out_specs=VMEM,
        out_shape=held(2 * H + 8, W),
        scratch_shapes=[pltpu.VMEM((W, D), f32)],
        compiler_params=limit(8),
        name="corner",
        cost_estimate=cost(10**6, 10**6),
    )(outside, near(planes))
    beside = across(corners, [(k, k ^ 1) for k in range(slabs)])
    rim = pl.pallas_call(
        pair_kernel,
        in_specs=[SMEM] + [VMEM] * 2,
        out_specs=VMEM,
        out_shape=held(H + 8, W),
        compiler_params=limit(8),
        name="pair",
        cost_estimate=cost(10**5, 10**5),
    )(par, near(corners), near(beside))
    far_rim = across(rim, [(k, k ^ 2) for k in range(slabs)])
    base = pl.pallas_call(
        nearly_kernel,
        in_specs=[SMEM, HBM, HBM, VMEM],
        out_specs=VMEM,
        out_shape=held(H, W, D),
        scratch_shapes=[pltpu.VMEM((2, W, D), f32), pltpu.SemaphoreType.DMA((NB,))],
        compiler_params=limit(8),
        name="nearly",
        cost_estimate=cost(10**8, 7 * 10**6),
    )(par, far(raw0), far(raw1), outside)
    return pl.pallas_call(
        final_kernel,
        in_specs=[SMEM] + [VMEM] * 10,
        out_specs=HBM,
        out_shape=pltpu.HBM((H, W, D), f32),
        scratch_shapes=[pltpu.VMEM((W, D), f32), *grid, pltpu.SemaphoreType.DMA((NB,))],
        compiler_params=limit(16),
        name="final",
        cost_estimate=cost(10**9, 13 * 10**6),
    )(
        par,
        near(base),
        near(fix),
        near(colm),
        near(corners),
        near(beside),
        near(rim),
        near(far_rim),
        near(u),
        near(hcol),
        near(spread),
    )


def solution(mesh):
    in_specs = (P("pencil", None, "slab"), P("pencil", None, "slab"), P(), P(), P(), P())
    out_specs = P("pencil", None, "slab")
    return jax.shard_map(per_device, mesh=mesh, in_specs=in_specs, out_specs=out_specs, check_vma=False)
```

```python
from functools import partial

import jax
import jax.numpy as jnp
from jax import lax
from jax.experimental import pallas as pl
from jax.experimental.pallas import tpu as pltpu
from jax.sharding import PartitionSpec as P

H, W, D = 16, 768, 128
B = 128
NB = W // B
NP = 32
S = W // NP
T = 32
HALF = 3
R = H + 8
f32 = jnp.float32
bf16 = jnp.bfloat16
HIGHEST = lax.Precision.HIGHEST


def log_decay(s):
    return jnp.log(2.0 * s / (1.0 + 2.0 * s + jnp.sqrt(1.0 + 4.0 * s)))


def pivots(log_r, length):
    return (
        jnp.exp(log_r)
        * (1.0 - jnp.exp(log_r * (2.0 * length)))
        / (1.0 - jnp.exp(log_r * (2.0 * length + 2.0)))
    )


def influence(log_r, m, i):
    return (
        jnp.exp(log_r * (i + 1.0))
        * (1.0 - jnp.exp(log_r * (2.0 * (m - i))))
        / (1.0 - jnp.exp(log_r * (2.0 * m + 2.0)))
    )


def green(s, log_r, n, i, j):
    low, high = jnp.minimum(i, j), jnp.maximum(i, j)
    return (
        jnp.exp(log_r * (high - low))
        * (1.0 - jnp.exp(log_r * (2.0 * low + 2.0)))
        * (1.0 - jnp.exp(log_r * (2.0 * (n - high))))
        / (jnp.sqrt(1.0 + 4.0 * s) * (1.0 - jnp.exp(log_r * (2.0 * n + 2.0))))
    )


def split(x):
    hi = x.astype(bf16)
    return hi, (x - hi.astype(f32)).astype(bf16)


def dot(a, b):
    return lax.dot_general(a, b, (((1,), (0,)), ((), ())), preferred_element_type=f32)


def iota(shape, dim):
    return lax.broadcasted_iota(jnp.int32, shape, dim)


HEAD, BEFORE_H, BEFORE_W, AH, CH, MH, PAIR = 0, 1, 5, 9, 10, 11, 12


def tables_kernel(cpl, slab, wi, di, par, cols, rows, gw3, gd4, spread, hmat, hcol, gwf, colm):
    row = (1, 128)
    sw, sh, sd = (jnp.full(row, cpl[k], f32) for k in range(3))
    lw, lh, ld = log_decay(sw), log_decay(sh), log_decay(sd)
    lane = iota(row, 1)
    k = lane.astype(f32)
    heads = [2.0 - 4.0 * sw - 4.0 * sd, 2.0 * sw, 2.0 * sd]
    for log_r, m in ((lw, float(B)), (lh, float(H)), (ld, float(D))):
        heads += [influence(log_r, m, 0.0), influence(log_r, m, m - 1.0)]
    middle = pivots(lh, float(H // 2))
    heads.append(1.0 / (1.0 - middle * middle))
    p, q = heads[7], heads[8]
    i1 = 1.0 / (1.0 - p * p)
    v = p + p * q * q * i1
    i2 = 1.0 / (1.0 - v * v)
    heads += [i2, i2 * v, jnp.full(row, lax.bitwise_and(slab[0], 1), jnp.int32).astype(f32)]
    one, none, two = jnp.ones(row, f32), jnp.zeros(row, f32), jnp.full(row, 2.0, f32)
    by_slab = (
        ((none, q * i1, q * i1 * p, one, none, none, none, none, two), (none,) * 5, (none, p * i1, i1, none, q * i1)),
        ((q * i1 * p, one, none, q * i1, none, none, two, none, none), (p * i1, none, none, i1, p * q * i1), (none,) * 4 + (one,)),
        ((one, q * i1 * p, q * i1, none, none, two, none, none, none), (none,) * 4 + (one,), (none, p * i1, i1, none, p * q * i1)),
        ((q * i1, none, one, q * i1 * p, none, none, none, two, none), (p * i1, none, none, i1, q * i1), (none,) * 5),
    )
    mine = jnp.full(row, slab[0], jnp.int32)
    for line in range(3):
        total = none
        for at in range(4):
            for n, value in enumerate(by_slab[at][line]):
                total = jnp.where((mine == at) & (lane == n), value, total)
        par[PAIR + line : PAIR + line + 1] = total
    head = jnp.zeros(row, f32)
    for at, v in enumerate(heads):
        head = jnp.where(lane == at, v, head)
    par[HEAD : HEAD + 1] = head
    for at, log_r, m, p, q in ((BEFORE_H, lh, float(H), heads[5], heads[6]), (BEFORE_W, lw, float(B), heads[3], heads[4])):
        before = pivots(log_r, m * k)
        inv = 1.0 / (1.0 - p * before)
        w = q * before * inv
        for n, v in enumerate((before, inv, w, q + w * p)):
            par[at + n : at + n + 1] = v
    kc = jnp.minimum(k, H - 1.0)
    ch = pivots(lh, kc + 1.0)
    par[AH : AH + 1] = influence(lh, float(H), kc)
    par[CH : CH + 1] = ch
    par[MH : MH + 1] = ch / sh
    tall = iota((B, D), 0).astype(f32)
    lww = jnp.broadcast_to(lw, (B, D))
    cols[0] = influence(lww, float(B), tall)
    cols[1] = influence(lww, float(B), B - 1.0 - tall)
    ca, cb = cols[0], cols[1]
    ca_hi, cb_hi = ca.astype(bf16).astype(f32), cb.astype(bf16).astype(f32)
    wide = iota((B, D), 1)
    mixed = jnp.where((wide == 0) | (wide == 8), ca_hi, jnp.where((wide == 1) | (wide == 9), cb_hi, 0.0))
    mixed = jnp.where(wide == 16, ca - ca_hi, jnp.where(wide == 17, cb - cb_hi, mixed))
    colm[...] = mixed[:, :32].astype(bf16)
    rows[0:1] = influence(lw, float(B), k)
    rows[1:2] = influence(lw, float(B), B - 1.0 - k)
    gwf[...] = wi[0]
    hi, lo = split(wi[0])
    gw3[:, :B] = hi
    gw3[:, B : 2 * B] = hi
    gw3[:, 2 * B :] = lo
    hi, lo = split(di[0].T)
    gd4[:D, :D] = hi
    gd4[:D, D:] = lo
    gd4[D:, :D] = hi
    gd4[D:, D:] = jnp.zeros((D, D), bf16)
    ad, bd = influence(ld, float(D), k), influence(ld, float(D), D - 1.0 - k)
    line = iota((2 * H, D), 0)
    for h in range(H):
        v = jnp.where(line == h, ad, jnp.where(line == H + h, bd, 0.0))
        hi, lo = split(v)
        at = slice(h * D, (h + 1) * D)
        spread[: 2 * H, at] = hi
        spread[2 * H : 4 * H, at] = hi
        spread[4 * H :, at] = lo
    a = iota((2 * H, 128), 0)
    b = iota((2 * H, 128), 1)
    af = lax.bitwise_and(a, H - 1).astype(f32)
    bfl = lax.bitwise_and(b, H - 1).astype(f32)
    wide_h = jnp.broadcast_to(lh, (2 * H, 128))
    g = green(jnp.broadcast_to(sh, (2 * H, 128)), wide_h, float(H), af, bfl)
    hmat[...] = jnp.where((b < 2 * H) & (lax.shift_right_logical(a, 4) == lax.shift_right_logical(b, 4)), g, 0.0)
    c = iota((H, 128), 0).astype(f32)
    ln = iota((H, 128), 1)
    hcol[...] = influence(jnp.broadcast_to(lh, (H, 128)), float(H), jnp.where(ln == 0, c, H - 1.0 - c))


def sums_kernel(cpl_far, rho, sig, cr, cs, own, comb, rv, sv, coef, packed, cpl, sems, sem):
    small = pltpu.make_async_copy(cpl_far, cpl, sem)
    small.start()
    def parts(i):
        at = pl.ds(pl.multiple_of(i * B, B), B)
        return (
            pltpu.make_async_copy(rho.at[:, at, :], rv.at[:, at, :], sems.at[0, i]),
            pltpu.make_async_copy(sig.at[:, at, :], sv.at[:, at, :], sems.at[1, i]),
        )

    for i in range(NB):
        for part in parts(i):
            part.start()
    small.wait()
    sh = jnp.full((8, 128), cpl[1], f32)
    lh = log_decay(sh)
    for h in range(H):
        coef[h] = influence(lh, float(H), float(h)) / sh

    R = 32
    lane = iota((R, D), 1)

    def block(i, _):
        for part in parts(i):
            part.wait()
        packs, combs = [], []
        for t in range(B // R):
            at = pl.ds(pl.multiple_of(i * B + t * R, R), R)
            fr = jnp.zeros((R, D), f32)
            tr, fs, ts, pack = fr, fr, fr, fr
            for h in range(H):
                x, y = rv[h, at, :], sv[h, at, :]
                cf = jnp.broadcast_to(coef[h, 0:1, :], (R, D))
                ct = jnp.broadcast_to(coef[H - 1 - h, 0:1, :], (R, D))
                fr, tr, fs, ts = fr + cf * x, tr + ct * x, fs + cf * y, ts + ct * y
                pack = jnp.where((lane == 2 * h) | (lane == 2 * h + 1), pltpu.roll(x, 2 * h + 1, 1), pack)
            cr[0, at, :], cr[1, at, :], cs[0, at, :], cs[1, at, :] = fr, tr, fs, ts
            packs.append(pack)
            combs.append(jnp.where(lane < 2, pltpu.roll(fr, 1, 1), pltpu.roll(tr, 3, 1)))
        at = pl.ds(pl.multiple_of(i * B, B), B)
        packed[...] = jnp.concatenate(packs, axis=0).T[: 2 * H]
        own[:H, at] = packed[pl.ds(1, H, stride=2), :]
        own[H:, at] = packed[pl.ds(0, H, stride=2), :]
        comb[:, at] = jnp.concatenate(combs, axis=0).T[:8]
        return 0

    lax.fori_loop(0, NB, block, 0)


def chain_w(yf, yt, par):
    p, q = par[HEAD, 3], par[HEAD, 4]
    before, inv, w, qw = (BEFORE_W + k for k in range(4))
    us = []
    for k in range(NB):
        u = yt[k] + par[w, k] * yf[k]
        us.append(u if k == 0 else u + par[qw, k] * us[-1])
    fs = [None] * NB
    for k in reversed(range(NB)):
        g = yf[k]
        if k > 0:
            g = g + p * us[k - 1]
        if k < NB - 1:
            g = g + q * fs[k + 1]
        fs[k] = g * par[inv, k]
    zero = jnp.zeros_like(yf[0])
    ls = [zero] + [us[k - 1] + par[before, k] * fs[k] for k in range(1, NB)]
    return ls, fs[1:] + [zero]


def solve_wd(x, gw3, gd4):
    hi, lo = split(x)
    z = dot(gw3[:, : 2 * B], jnp.concatenate([hi, lo], axis=0)) + dot(gw3[:, 2 * B :], hi)
    z = jnp.concatenate([z[:, :D], z[:, D:]], axis=0)
    hi, lo = split(z)
    y = dot(jnp.concatenate([hi, lo], axis=1), gd4[...])
    return y[:, :D] + y[:, D:]


def edges_kernel(par, cr, cs, comb, gwf, rows, gw3, gd4, cols, out, e, wc):
    c0, c1, c2 = par[HEAD, 0], par[HEAD, 1], par[HEAD, 2]
    row = iota((B, D), 0)
    parts = []
    for k in range(NB):
        spot = slice(k * B, (k + 1) * B)
        xs = []
        for j in range(2):
            x = cr[j, spot]
            up = pltpu.roll(x, 1, 0)
            up = jnp.where(row == 0, cr[j, k * B - 1 : k * B] if k > 0 else 0.0, up)
            down = pltpu.roll(x, B - 1, 0)
            down = jnp.where(row == B - 1, cr[j, (k + 1) * B : (k + 1) * B + 1] if k < NB - 1 else 0.0, down)
            xs.append(cs[j, spot] + c0 * x + c1 * (up + down) + c2 * (pltpu.roll(x, 1, 1) + pltpu.roll(x, D - 1, 1)))
        y = solve_wd(jnp.concatenate(xs, axis=1), gw3, gd4)
        e[0, spot] = y[:B]
        e[1, spot] = y[B:]
        parts.append(
            lax.dot_general(
                comb[:, spot], gwf[...], (((1,), (1,)), ((), ())), precision=HIGHEST, preferred_element_type=f32
            )
        )
    ls, rs = chain_w([a[:, 0:1] for a in parts], [a[:, B - 1 : B] for a in parts], par)
    for k in range(NB):
        wc[:, k * B : (k + 1) * B] = parts[k] + ls[k] * rows[0:1] + rs[k] * rows[1:2]
    line = wc[...]
    for p in range(NP):
        out[p, 2 * S :] = pltpu.roll(line, (W - S * p) % W, 1)[:, :D]
    for j in range(2):
        ls, rs = chain_w(
            [e[j, k * B : k * B + 1] for k in range(NB)], [e[j, k * B + B - 1 : k * B + B] for k in range(NB)], par
        )
        for k in range(NB):
            spot = slice(k * B, (k + 1) * B)
            e[j, spot] = e[j, spot] + cols[0] * ls[k] + cols[1] * rs[k]
        for p in range(NP):
            out[p, S * j : S * (j + 1)] = e[j, S * p : S * (p + 1)]


def field_kernel(start, count, par, rho, sig, gw3, gd4, raw, ew, qp, rv, out, packed, sems, rims):
    sv = out

    def place(i, lead=0):
        return pl.ds(pl.multiple_of(i * B + lead, 8), B)

    def parts(i):
        there = place(i, start * B)
        return (
            pltpu.make_async_copy(rho.at[:, there, :], rv.at[:, place(i, 8), :], sems.at[0, i]),
            pltpu.make_async_copy(sig.at[:, there, :], out.at[:, place(i), :], sems.at[1, i]),
        )

    def send(i):
        return pltpu.make_async_copy(out.at[:, place(i), :], raw.at[:, place(i), :], sems.at[2, i])

    ends = []
    if start > 0:
        ends.append((start * B - 8, 0))
    if start + count < NB:
        ends.append(((start + count) * B, 8 + count * B))
    ends = [
        pltpu.make_async_copy(rho.at[:, pl.ds(there, 8), :], rv.at[:, pl.ds(here, 8), :], rims.at[n])
        for n, (there, here) in enumerate(ends)
    ]
    for end in ends:
        end.start()
    for i in range(count):
        for part in parts(i):
            part.start()
    for end in ends:
        end.wait()
    for part in parts(0):
        part.wait()
    c0, c1, c2 = par[HEAD, 0], par[HEAD, 1], par[HEAD, 2]
    row = iota((B, D), 0)
    half = H // 2
    meet = par[HEAD, 9]

    def block(i, _):
        @pl.when(i < count - 1)
        def _():
            for part in parts(jnp.minimum(i + 1, count - 1)):
                part.wait()

        here = place(i)
        inner = place(i, 8)
        before = pl.ds(pl.multiple_of(i * B, 8), 8)
        after = pl.ds(pl.multiple_of(i * B + B + 8, 8), 8)
        for h in range(H):
            x = rv[h, inner, :]
            first = jnp.where(i + start > 0, rv[h, before, :][7:8], 0.0)
            last = jnp.where(i + start < NB - 1, rv[h, after, :][0:1], 0.0)
            up = jnp.where(row == 0, first, pltpu.roll(x, 1, 0))
            down = jnp.where(row == B - 1, last, pltpu.roll(x, B - 1, 0))
            out[h, here, :] = (
                sv[h, here, :] + c0 * x + c1 * (up + down) + c2 * (pltpu.roll(x, 1, 1) + pltpu.roll(x, D - 1, 1))
            )

        def tile(j, _):
            at = pl.ds(pl.multiple_of(i * B + T * j, T), T)
            beside = pl.ds(pl.multiple_of(i * B + T * j + 8, 8), T)
            top, bottom = [None] * half, [None] * half
            for h in range(half):
                m, c = par[MH, h], par[CH, h]
                a, b = m * out[h, at, :], m * out[H - 1 - h, at, :]
                top[h] = a if h == 0 else a + c * top[h - 1]
                bottom[h] = b if h == 0 else b + c * bottom[h - 1]
            c = par[CH, half - 1]
            x = (top[half - 1] + c * bottom[half - 1]) * meet
            y = bottom[half - 1] + c * x
            for h in reversed(range(half)):
                if h < half - 1:
                    c = par[CH, h]
                    x, y = top[h] + c * x, bottom[h] + c * y
                out[h, at, :] = x - 2.0 * rv[h, beside, :]
                out[H - 1 - h, at, :] = y - 2.0 * rv[H - 1 - h, beside, :]
            return 0

        lax.fori_loop(0, B // T, tile, 0)
        lane = iota((B, D), 1)
        pack = jnp.zeros((B, D), f32)
        for g in range(H // 2):
            y = solve_wd(jnp.concatenate([out[2 * g, here, :], out[2 * g + 1, here, :]], axis=1), gw3, gd4)
            for side in range(2):
                h = 2 * g + side
                part = y[side * B : (side + 1) * B]
                ew[i, 0, h : h + 1, :] = part[0:1]
                ew[i, 1, h : h + 1, :] = part[B - 1 : B]
                out[h, here, :] = part + rv[h, inner, :]
                pack = jnp.where((lane == 2 * h) | (lane == 2 * h + 1), pltpu.roll(part, 2 * h + 1, 1), pack)
        packed[...] = pack.T[: 2 * H]
        qp[:H, here] = packed[pl.ds(1, H, stride=2), :]
        qp[H:, here] = packed[pl.ds(0, H, stride=2), :]
        send(i).start()
        return 0

    lax.fori_loop(0, count, block, 0)
    for i in range(count):
        send(i).wait()


def planes_kernel(par, ew0, ew1, qp0, qp1, own, hmat, rows, gwf, planes, fix, flat):
    ew = [ew0[k] for k in range(HALF)] + [ew1[k] for k in range(NB - HALF)]
    ls, rs = chain_w([a[0] for a in ew], [a[1] for a in ew], par)
    flat[...] = jnp.zeros((8, H * D), f32)
    for k in range(NB):
        for h in range(H):
            flat[0:1, h * D : (h + 1) * D] = ls[k][h : h + 1]
            flat[1:2, h * D : (h + 1) * D] = rs[k][h : h + 1]
        x = flat[...]
        hi = x.astype(bf16).astype(f32)
        fix[k] = jnp.concatenate([hi, x - hi, hi, jnp.zeros_like(x)], axis=0).astype(bf16)
    v = jnp.dot(hmat[:, : 2 * H], own[...], precision=HIGHEST, preferred_element_type=f32)
    parts = []
    for k in range(NB):
        spot = slice(k * B, (k + 1) * B)
        solved = lax.dot_general(
            v[:, spot], gwf[...], (((1,), (1,)), ((), ())), precision=HIGHEST, preferred_element_type=f32
        )
        seen = qp0[:, spot] if k < HALF else qp1[:, (k - HALF) * B : (k - HALF + 1) * B]
        parts.append(jnp.concatenate([seen, solved], axis=0))
    ls, rs = chain_w([a[:, 0:1] for a in parts], [a[:, B - 1 : B] for a in parts], par)
    for k in range(NB):
        planes[:, k * B : (k + 1) * B] = parts[k] + ls[k] * rows[0:1] + rs[k] * rows[1:2]


def groups(ref):
    return [ref[R * k : R * (k + 1)] for k in range(4)]


def pair_kernel(par, a, b, known, rim):
    p, q = 2.0 * par[HEAD, 7], 2.0 * par[HEAD, 8]
    odd = par[HEAD, 12]
    even = 1.0 - odd
    f, t, h0, h1 = groups(a)
    f2, t2, g0, g1 = groups(b)
    f = f - p * h1 - q * h0 + (even * q) * g0 + (odd * p) * g1
    t = t - q * h1 - p * h0 + (even * p) * g0 + (odd * q) * g1
    f2 = f2 - p * g1 - q * g0 + (odd * q) * h0 + (even * p) * h1
    t2 = t2 - q * g1 - p * g0 + (odd * p) * h0 + (even * q) * h1
    total = par[PAIR, 5] * h0 + par[PAIR, 6] * h1 + par[PAIR, 7] * g0 + par[PAIR, 8] * g1
    for k, v in enumerate((f, t, f2, t2)):
        known[R * k : R * (k + 1)] = v
        total = total + par[PAIR, k] * v
    rim[...] = total


def solver_kernel(par, y, out, us, uc):
    p, q = par[HEAD, 5], par[HEAD, 6]
    before, inv, w, qw = (BEFORE_H + k for k in range(4))
    row = iota((8, D), 0)

    def lines(k):
        c = y[k, 2 * S :]
        return (y[k, :S], y[k, S : 2 * S]), (c, pltpu.roll(c, 6, 0))

    u = [None, None]
    for k in range(NP):
        for n, (first, last) in enumerate(lines(k)):
            v = last + par[w, k] * first
            u[n] = v if k == 0 else v + par[qw, k] * u[n]
        us[k] = u[0]
        uc[k] = u[1]
    f = [jnp.zeros((S, D), f32), jnp.zeros((8, D), f32)]
    for k in reversed(range(NP)):
        beyond = list(f)
        inside = [None, None]
        for n, (first, _) in enumerate(lines(k)):
            g = first
            held_u = (us, uc)[n][k - 1] if k > 0 else None
            if k > 0:
                g = g + p * held_u
            f[n] = (g + q * f[n]) * par[inv, k]
            inside[n] = held_u + par[before, k] * f[n] if k > 0 else jnp.zeros_like(f[n])
        out[k, :S] = inside[0]
        out[k, S : 2 * S] = beyond[0]
        out[k, 2 * S :] = jnp.where(row < 2, inside[1], pltpu.roll(beyond[1], 2, 0))


def corner_kernel(a, planes, out, wide):
    for k in range(4):
        out[R * k : R * k + H] = planes[H * k : H * (k + 1)]
    lane = iota((S, D), 1)
    narrow = iota((8, D), 1)
    line = jnp.zeros((8, W), f32)
    blank = jnp.zeros((8, W - D), f32)
    for p in range(NP):
        l, r = a[p, :S], a[p, S : 2 * S]
        v = jnp.where(lane == 0, l, jnp.where(lane == 1, pltpu.roll(r, 1, 1), 0.0))
        wide[S * p : S * (p + 1)] = jnp.where(
            lane == 8, pltpu.roll(l, 9, 1), jnp.where(lane == 9, pltpu.roll(r, 10, 1), v)
        )
        piece = jnp.concatenate([jnp.where(narrow < S, a[p, 2 * S :], 0.0), blank], axis=1)
        line = line + pltpu.roll(piece, S * p, 1)
    row = iota((8, W), 0)
    out[2 * R + H : 3 * R] = jnp.where(
        row == 0, pltpu.roll(line, 7, 0), jnp.where(row == 1, pltpu.roll(line, 6, 0), 0.0)
    )
    out[3 * R + H :] = jnp.where(row == 0, line, jnp.where(row == 1, pltpu.roll(line, 7, 0), 0.0))
    for k in range(NB):
        spot = slice(k * B, (k + 1) * B)
        both = wide[spot].T[:16]
        out[H:R, spot] = both[:8]
        out[R + H : 2 * R, spot] = both[8:]


def nearly_kernel(par, raw0, raw1, a, out, lr, sems):
    for i in range(NB):
        raw, k = (raw0, i) if i < HALF else (raw1, i - HALF)
        spot = pl.ds(i * B, B)
        pltpu.make_async_copy(raw.at[:, pl.ds(k * B, B), :], out.at[:, spot, :], sems.at[i]).start()
    for p in range(NP):
        for j in range(2):
            lr[j, S * p : S * (p + 1)] = a[p, S * j : S * (j + 1)]

    def block(i, _):
        at = pl.ds(pl.multiple_of(i * B, B), B)
        pltpu.make_async_copy(raw1.at[:, pl.ds(0, B), :], out.at[:, at, :], sems.at[i]).wait()
        l, r = lr[0, at, :], lr[1, at, :]
        for h in range(H):
            out[h, at, :] = out[h, at, :] + (par[AH, h] * l + par[AH, H - 1 - h] * r)
        return 0

    lax.fori_loop(0, NB, block, 0)


def final_kernel(par, base, fix, colm, a, b, parts, v0, v1, hcol, spread, out, tall, buf, sems):
    beyond = par[HEAD, 10] * v1[...] + par[HEAD, 11] * v0[...]
    odd = par[HEAD, 12]
    even = 1.0 - odd
    _, _, h0, h1 = groups(a)
    _, _, g0, g1 = groups(b)
    sides = []
    for side, start in enumerate(((2.0 * odd) * g1 - 2.0 * h1, (2.0 * even) * g0 - 2.0 * h0)):
        total = start + par[PAIR + 1 + side, 4] * beyond
        for k, part in enumerate(groups(parts)):
            total = total + par[PAIR + 1 + side, k] * part
        sides.append(total[:H] + hcol[:, 0:1] * total[H : H + 1] + hcol[:, 1:2] * total[H + 1 : H + 2])
    both = jnp.concatenate(sides + [jnp.zeros((D - 2 * H, W), f32)], axis=0)
    for k in range(NB):
        tall[k * B : (k + 1) * B] = both[:, k * B : (k + 1) * B].T

    def send(i):
        at = pl.ds(pl.multiple_of(i * B, B), B)
        return pltpu.make_async_copy(buf.at[:, at, :], out.at[:, at, :], sems.at[i])

    def block(i, _):
        at = pl.ds(pl.multiple_of(i * B, B), B)
        hi, lo = split(tall[at, : 2 * H])
        wide = dot(
            jnp.concatenate([hi, lo, hi, colm[...]], axis=1), jnp.concatenate([spread[...], fix[i]], axis=0)
        )
        for h in range(H):
            buf[h, at, :] = base[h, at, :] + wide[:, h * D : (h + 1) * D]
        send(i).start()
        return 0

    lax.fori_loop(0, NB, block, 0)
    for i in range(NB):
        send(i).wait()


SMEM = pl.BlockSpec(memory_space=pltpu.SMEM)
VMEM = pl.BlockSpec(memory_space=pltpu.VMEM)
HBM = pl.BlockSpec(memory_space=pltpu.HBM)


def limit(mib):
    return pltpu.CompilerParams(vmem_limit_bytes=mib * 2**20)


def held(*shape, dtype=f32):
    return pltpu.VMEM(shape, dtype)


def near(x):
    return pltpu.with_memory_space_constraint(x, pltpu.VMEM)


def far(x):
    return pltpu.with_memory_space_constraint(x, pltpu.HBM)


def cost(flops, bytes_accessed):
    return pl.CostEstimate(flops=flops, bytes_accessed=bytes_accessed, transcendentals=0)


def per_device(density, source, coupling, width_inverse, height_inverse, depth_inverse):
    slab = lax.axis_index("slab")
    slabs = lax.axis_size("slab")

    def across(value, pairs):
        return lax.ppermute(value, "slab", pairs)

    grid = [pltpu.VMEM((H, W + 8, D), f32)]

    cr, cs, own, comb = pl.pallas_call(
        sums_kernel,
        in_specs=[HBM] * 3,
        out_specs=[VMEM] * 4,
        out_shape=[held(2, W, D), held(2, W, D), held(2 * H, W), held(8, W)],
        scratch_shapes=grid * 2
        + [
            pltpu.VMEM((H, 8, 128), f32),
            pltpu.VMEM((2 * H, B), f32),
            pltpu.SMEM((3,), f32),
            pltpu.SemaphoreType.DMA((2, NB)),
            pltpu.SemaphoreType.DMA(()),
        ],
        compiler_params=limit(24),
        name="sums",
        cost_estimate=cost(10**7, 14 * 10**6),
    )(far(coupling), far(density), far(source))
    first = pl.BlockSpec((1, B, B), lambda *_: (0, 0, 0))
    shapes = [
        ((16, 128), f32),
        ((2, B, D), f32),
        ((8, 128), f32),
        ((B, 3 * B), bf16),
        ((2 * D, 2 * D), bf16),
        ((6 * H, H * D), bf16),
        ((2 * H, 128), f32),
        ((H, 128), f32),
        ((B, B), f32),
        ((B, 32), bf16),
    ]
    par, cols, rows, gw3, gd4, spread, hmat, hcol, gwf, colm = pl.pallas_call(
        tables_kernel,
        grid=(1,),
        in_specs=[SMEM, SMEM, first, first],
        out_specs=[pl.BlockSpec(shape, lambda *_, n=len(shape): (0,) * n) for shape, _ in shapes],
        out_shape=[jax.ShapeDtypeStruct(*shapes[0])] + [held(*shape, dtype=kind) for shape, kind in shapes[1:]],
        compiler_params=limit(8),
        name="tables",
        cost_estimate=cost(10**7, 10**6),
    )(coupling, slab.reshape(1), width_inverse, depth_inverse)

    edges = pl.pallas_call(
        edges_kernel,
        in_specs=[SMEM] + [VMEM] * 8,
        out_specs=VMEM,
        out_shape=held(NP, 2 * S + 8, D),
        scratch_shapes=[pltpu.VMEM((2, W, D), f32), pltpu.VMEM((8, W), f32)],
        compiler_params=limit(8),
        name="edges",
        cost_estimate=cost(10**8, 3 * 10**6),
    )(par, near(cr), near(cs), near(comb), near(gwf), near(rows), near(gw3), near(gd4), near(cols))
    arrived = lax.all_to_all(edges, "pencil", 0, 0, tiled=True)

    def field(start, count):
        rows = count * B
        return pl.pallas_call(
            partial(field_kernel, start, count),
            in_specs=[SMEM, HBM, HBM, VMEM, VMEM],
            out_specs=[HBM, VMEM, VMEM],
            out_shape=[pltpu.HBM((H, rows, D), f32), held(count, 2, H, D), held(2 * H, rows)],
            scratch_shapes=[
                pltpu.VMEM((H, rows + 16, D), f32),
                pltpu.VMEM((H, rows, D), f32),
                pltpu.VMEM((2 * H, B), f32),
                pltpu.SemaphoreType.DMA((3, count)),
                pltpu.SemaphoreType.DMA((2,)),
            ],
            compiler_params=limit(24),
            name="field" + str(start),
            cost_estimate=cost(2 * 10**9, 10**7),
        )(par, far(density), far(source), near(gw3), near(gd4))

    raw0, ew0, qp0 = field(0, HALF)
    arrived, ew0 = lax.optimization_barrier((arrived, ew0))
    solved = pl.pallas_call(
        solver_kernel,
        in_specs=[SMEM, VMEM],
        out_specs=VMEM,
        out_shape=held(NP, 2 * S + 8, D),
        scratch_shapes=[pltpu.VMEM((NP, S, D), f32), pltpu.VMEM((NP, 8, D), f32)],
        compiler_params=limit(8),
        name="solver",
        cost_estimate=cost(10**6, 2 * 10**6),
    )(par, near(arrived))
    outside = lax.all_to_all(solved, "pencil", 0, 0, tiled=True)

    raw1, ew1, qp1 = field(HALF, NB - HALF)
    planes, fix = pl.pallas_call(
        planes_kernel,
        in_specs=[SMEM] + [VMEM] * 8,
        out_specs=[VMEM] * 2,
        out_shape=[held(4 * H, W), held(NB, 32, H * D, dtype=bf16)],
        scratch_shapes=[pltpu.VMEM((8, H * D), f32)],
        compiler_params=limit(8),
        name="planes",
        cost_estimate=cost(10**8, 10**6),
    )(par, *[near(v) for v in (ew0, ew1, qp0, qp1)], near(own), near(hmat), near(rows), near(gwf))

    outside = near(outside)
    corners = pl.pallas_call(
        corner_kernel,
        in_specs=[VMEM] * 2,
        out_specs=VMEM,
        out_shape=held(4 * R, W),
        scratch_shapes=[pltpu.VMEM((W, D), f32)],
        compiler_params=limit(8),
        name="corner",
        cost_estimate=cost(10**6, 10**6),
    )(outside, near(planes))
    beside = across(corners, [(k, k ^ 1) for k in range(slabs)])
    parts, rim = pl.pallas_call(
        pair_kernel,
        in_specs=[SMEM] + [VMEM] * 2,
        out_specs=[VMEM] * 2,
        out_shape=[held(4 * R, W), held(R, W)],
        compiler_params=limit(8),
        name="pair",
        cost_estimate=cost(10**5, 10**5),
    )(par, near(corners), near(beside))
    far_rim = across(rim, [(k, k ^ 2) for k in range(slabs)])
    base = pl.pallas_call(
        nearly_kernel,
        in_specs=[SMEM, HBM, HBM, VMEM],
        out_specs=VMEM,
        out_shape=held(H, W, D),
        scratch_shapes=[pltpu.VMEM((2, W, D), f32), pltpu.SemaphoreType.DMA((NB,))],
        compiler_params=limit(8),
        name="nearly",
        cost_estimate=cost(10**8, 7 * 10**6),
    )(par, far(raw0), far(raw1), outside)
    return pl.pallas_call(
        final_kernel,
        in_specs=[SMEM] + [VMEM] * 10,
        out_specs=HBM,
        out_shape=pltpu.HBM((H, W, D), f32),
        scratch_shapes=[pltpu.VMEM((W, D), f32), *grid, pltpu.SemaphoreType.DMA((NB,))],
        compiler_params=limit(16),
        name="final",
        cost_estimate=cost(10**9, 13 * 10**6),
    )(
        par,
        near(base),
        near(fix),
        near(colm),
        near(corners),
        near(beside),
        near(parts),
        near(rim),
        near(far_rim),
        near(hcol),
        near(spread),
    )


def solution(mesh):
    in_specs = (P("pencil", None, "slab"), P("pencil", None, "slab"), P(), P(), P(), P())
    out_specs = P("pencil", None, "slab")
    return jax.shard_map(per_device, mesh=mesh, in_specs=in_specs, out_specs=out_specs, check_vma=False)
```
